8 devices in a mesh: dp: 1 (over z), vp: 8 (over y, x, core).
Axes of the slice: x: 2, y: 2, z: 1, core: 2. Of those that a mesh axis runs over, the one named last changes fastest.
Arguments:
- hidden: bfloat16 [2048, 2048], P(('dp', 'vp'))
- labels: int32 [2048], P(('dp', 'vp'))
- loss_weight: float32 [2048], P(('dp', 'vp'))
- norm_gain: float32 [2048], replicated
- w_unembed: bfloat16 [2048, 32128], P(None, 'vp')
Outputs:
- output 1: float32 [1], P('dp')
- output 2: bfloat16 [2048, 2048], P(('dp', 'vp'))
- output 3: float32 [2048, 32128], P('dp', 'vp')
- output 4: float32 [2048], P('dp')
All inputs are finite; a program needn't handle non-finite values.
Results may differ from the reference program's by a relative error of at most 0.001.
Values are sent between devices in bfloat16 or wider.
A program may use at most 1 GiB of HBM per device.

```python
import jax
import jax.numpy as jnp
from jax import lax

D = 2048
V = 32000
PAD_COLS = 128
TOK_DEV = 256
GROUP_SIZE = 8
VOCAB_PAD = V + PAD_COLS
TOKENS = TOK_DEV * GROUP_SIZE
LOW_IDS = V // 64
NORM_EPS = 1e-5


def setup_inputs(seed: int = 0, part: int = 0) -> dict:
    base_key = jax.random.key(seed)
    shared_key, parts_key = jax.random.split(base_key)
    part_key = jax.random.fold_in(parts_key, part)
    key_hid, key_pick, key_low, key_any, key_pad, key_wt = jax.random.split(part_key, 6)
    key_gain, key_unemb = jax.random.split(shared_key)
    hidden = jax.random.normal(key_hid, (TOKENS, D), jnp.float32).astype(jnp.bfloat16)
    tok_ids = jnp.arange(TOKENS)
    pick_low = jax.random.randint(key_pick, (TOKENS,), 0, 2)
    low_ids = jax.random.randint(key_low, (TOKENS,), 0, LOW_IDS)
    any_ids = jax.random.randint(key_any, (TOKENS,), 0, V)
    labels = jnp.where(pick_low == 0, low_ids, any_ids)
    labels = jnp.where(tok_ids == TOKENS - 1, V - 1, labels).astype(jnp.int32)
    pad_draw = jax.random.randint(key_pad, (TOKENS,), 0, 8)
    is_pad = (pad_draw == 0) & (tok_ids > 0)
    weight_val = jax.random.uniform(key_wt, (TOKENS,), jnp.float32, 0.25, 1.75)
    loss_weight = jnp.where(is_pad, 0.0, weight_val).astype(jnp.float32)
    norm_gain = 1.0 + 0.25 * jax.random.normal(key_gain, (D,), jnp.float32)
    w_unembed = (jax.random.normal(key_unemb, (D, VOCAB_PAD), jnp.float32) * (2.0 * D ** -0.5)).astype(jnp.bfloat16)
    return {"hidden": hidden, "labels": labels, "loss_weight": loss_weight, "norm_gain": norm_gain, "w_unembed": w_unembed}


def reference(hidden, labels, loss_weight, norm_gain, w_unembed):
    x_float = hidden.astype(jnp.float32)
    inv_rms = lax.rsqrt(jnp.mean(x_float * x_float, axis=-1, keepdims=True) + NORM_EPS)
    x_norm = x_float * inv_rms
    normed = (x_norm * norm_gain).astype(jnp.bfloat16)
    tok_scale = loss_weight / jnp.sum(loss_weight)
    col_ids = jnp.arange(VOCAB_PAD)[None, :]

    def block_step(d_unembed, block_in):
        normed_blk, label_blk, scale_blk = block_in
        logits = jnp.dot(normed_blk, w_unembed, preferred_element_type=jnp.float32)
        logits = jnp.where(col_ids < V, logits, -jnp.inf)
        is_target = col_ids == label_blk[:, None]
        row_max = jnp.max(logits, axis=1, keepdims=True)
        log_norm = row_max + jnp.log(jnp.sum(jnp.exp(logits - row_max), axis=1, keepdims=True))
        target = jnp.sum(jnp.where(is_target, logits, 0.0), axis=1, keepdims=True)
        tok_loss = (log_norm - target)[:, 0] * scale_blk
        d_logits = ((jnp.exp(logits - log_norm) - jnp.where(is_target, 1.0, 0.0)) * scale_blk[:, None]).astype(jnp.bfloat16)
        d_unembed = d_unembed + jnp.dot(normed_blk.T, d_logits, preferred_element_type=jnp.float32)
        d_normed = jnp.dot(d_logits, w_unembed.T, preferred_element_type=jnp.float32)
        return d_unembed, (tok_loss, d_normed)

    blocks = (normed.reshape(GROUP_SIZE, TOK_DEV, D), labels.reshape(GROUP_SIZE, TOK_DEV), tok_scale.reshape(GROUP_SIZE, TOK_DEV))
    d_unembed, (tok_loss, d_normed) = lax.scan(block_step, jnp.zeros((D, VOCAB_PAD), jnp.float32), blocks)
    d_normed = d_normed.reshape(TOKENS, D)
    mean_loss = jnp.sum(tok_loss).reshape(1)
    grad_hat = d_normed * norm_gain
    d_input = inv_rms * (grad_hat - x_norm * jnp.mean(grad_hat * x_norm, axis=-1, keepdims=True))
    d_norm_gain = jnp.sum(d_normed * x_norm, axis=0)
    return mean_loss, d_input.astype(jnp.bfloat16), d_unembed, d_norm_gain
```

```python
import functools

import jax
import jax.numpy as jnp
from jax import lax
from jax.experimental import pallas as pl
from jax.experimental.pallas import tpu as pltpu
from jax.sharding import PartitionSpec as P

NORM_EPS = 1e-5
PAD_COLS = 128
LANES = 128
VT = 1024
NT = 1024
LOWEST = -3.0e38
MESH = pl.DeviceIdType.MESH
VMEM_BYTES = 67_000_000


def xor_peers(me):
    step_core = 1 - 2 * (me % 2)
    step_x = 2 - 4 * ((me // 2) % 2)
    step_y = 4 - 8 * (me // 4)
    return [me + (r % 2) * step_core + ((r // 2) % 2) * step_x + (r // 4) * step_y for r in range(8)]


def unit_of(rel, half):
    if rel in (0, 1):
        return 2 * rel + half
    if rel in (6, 7):
        return 12 + 2 * (rel - 6) + half
    return {2: 4, 4: 5, 3: 6, 5: 7}[rel] + 4 * half


def head_kernel(
    hidden_hbm, meta_ref, gain_ref, w_hbm,
    a_out, dz_out, px_out, py_out, pown_out, z_hbm, loss_ref,
    w_v, a_v, z_v, dz_v, meta_v, row_v, m_v, s_v, t_v, st_v, out_v, prt_v, drecv_v, dsend_v, hold_v, stage_v,
    ag_send, ag_recv, meta_send, meta_recv, st_send, st_recv, prt_send, prt_recv, d_send, d_recv,
    in_sem, w_sem, z_sem, a_sem, dz_sem, stage_sem, fin_sem, credit,
):
    me = lax.axis_index("vp")
    peers = xor_peers(me)
    vocab_local, width = w_hbm.shape
    vocab_real = 8 * vocab_local - PAD_COLS
    padded = w_v.shape[0]
    n_vt = padded // VT
    tok_dev = hidden_hbm.shape[0]
    chunk = 2 * tok_dev
    half = tok_dev // 2
    mine = tok_dev

    def remote(src, dst, send, recv, rel):
        return pltpu.make_async_remote_copy(
            src_ref=src, dst_ref=dst, send_sem=send, recv_sem=recv,
            device_id={"vp": peers[rel]}, device_id_type=MESH,
        )

    hidden_v = dz_v.at[0, 0:tok_dev, 0:width]
    hidden_copy = pltpu.make_async_copy(hidden_hbm, hidden_v, in_sem)
    hidden_copy.start()
    barrier = pltpu.get_barrier_semaphore()
    for r in range(1, 8):
        pl.semaphore_signal(barrier, inc=1, device_id={"vp": peers[r]}, device_id_type=MESH)

    def w_copy(j):
        hi = min((j + 1) * VT, vocab_local)
        return pltpu.make_async_copy(w_hbm.at[j * VT:hi], w_v.at[j * VT:hi], w_sem.at[j])

    for j in range(n_vt):
        w_copy(j).start()
    meta_v[0] = meta_ref[...]

    hidden_copy.wait()
    for b in range(0, tok_dev, 32):
        x = dz_v[0, b:b + 32, 0:width].astype(jnp.float32)
        inv_rms = lax.rsqrt(jnp.mean(x * x, axis=-1, keepdims=True) + NORM_EPS)
        a_v[b:b + 32, :] = (x * inv_rms * gain_ref[...]).astype(jnp.bfloat16)
    w_v[vocab_local:padded, :] = jnp.zeros((padded - vocab_local, width), jnp.bfloat16)
    pl.semaphore_wait(barrier, 7)

    metas = [remote(meta_v.at[0], meta_v.at[r], meta_send.at[r - 1], meta_recv.at[r - 1], r) for r in range(1, 8)]
    for copy in metas:
        copy.start()

    def ag(idx, src, dst, count, rel):
        return remote(
            a_v.at[src:src + count], a_v.at[dst:dst + count], ag_send.at[idx], ag_recv.at[idx], rel
        )

    c1, c2, c3 = chunk, 2 * chunk, 3 * chunk
    own_p = ag(0, 0, mine, mine, 1)
    x_h0 = ag(1, 0, c1, half, 2)
    y_h0 = ag(2, 0, c1 + half, half, 4)
    m1_p = ag(3, c1, c1 + mine, mine, 1)
    x_h1 = ag(4, half, c2, half, 2)
    y_h1 = ag(5, half, c2 + half, half, 4)
    m2_p = ag(6, c2, c2 + mine, mine, 1)
    d_h0 = ag(7, c1 + half, c3, half, 2)
    d_h1 = ag(8, c2, c3 + half, half, 4)
    d_p = ag(9, c3, c3 + mine, mine, 1)
    for copy in (x_h0, y_h0, own_p, x_h1, y_h1):
        copy.start()

    for copy in metas:
        copy.wait_recv()
    for rel in range(8):
        for h in range(2):
            u = unit_of(rel, h)
            row_v[:, u * LANES:(u + 1) * LANES] = meta_v[rel, :, h * LANES:(h + 1) * LANES]

    base_f = (me * vocab_local).astype(jnp.float32)
    local = row_v[0:1, :] - base_f
    row_v[0:1, :] = jnp.where(local < float(vocab_local), local, -1.0)
    valid = jnp.minimum(vocab_local, vocab_real - me * vocab_local)

    def chunk_at(c):
        return pl.ds(pl.multiple_of(c * chunk, chunk), chunk)

    def row_at(row, c, lt):
        return row_v[row:row + 1, pl.ds(pl.multiple_of(c * chunk + lt * LANES, LANES), LANES)]

    def a_copy(c):
        return pltpu.make_async_copy(a_v.at[chunk_at(c)], a_out.at[chunk_at(c)], a_sem.at[c])

    def z_copy(t):
        return pltpu.make_async_copy(z_v.at[t % 4], z_hbm.at[t], z_sem.at[t % 4])

    group = 256
    sub_f = lax.broadcasted_iota(jnp.int32, (8, LANES), 0).astype(jnp.float32)
    step_f = 8.0 * lax.broadcasted_iota(jnp.int32, (group // 8, 8, LANES), 0).astype(jnp.float32)

    def stats_pass(c, j):
        first = j == 0
        for lt in range(chunk // LANES):
            cols = slice(lt * LANES, (lt + 1) * LANES)
            lab = row_at(0, c, lt) - (j * VT).astype(jnp.float32) - sub_f
            m = jnp.where(first, LOWEST, m_v[:, cols])
            s = jnp.where(first, 0.0, s_v[:, cols])
            t = jnp.where(first, 0.0, t_v[:, cols])
            for b in range(0, VT, group):
                z = z_v[j, b:b + group, cols].reshape(group // 8, 8, LANES)
                m_new = jnp.maximum(m, jnp.max(z, axis=0))
                s = s * jnp.exp(m - m_new) + jnp.sum(jnp.exp(z - m_new[None]), axis=0)
                t += jnp.sum(jnp.where((lab - float(b))[None] == step_f, z, 0.0), axis=0)
                m = m_new
            m_v[:, cols] = m
            s_v[:, cols] = s
            t_v[:, cols] = t

    def st_copy(c, r):
        at = (slice(None), chunk_at(c))
        return remote(st_v.at[(0, *at)], st_v.at[(r, *at)], st_send.at[c * 7 + r - 1], st_recv.at[c * 7 + r - 1], r)

    def send_stats(c):
        m = m_v[...]
        m_row = jnp.max(m, axis=0, keepdims=True)
        st_v[0, 0:1, chunk_at(c)] = m_row
        st_v[0, 1:2, chunk_at(c)] = jnp.sum(s_v[...] * jnp.exp(m - m_row), axis=0, keepdims=True)
        st_v[0, 2:3, chunk_at(c)] = jnp.sum(t_v[...], axis=0, keepdims=True)
        for r in range(1, 8):
            st_copy(c, r).start()

    st_v[0] = jnp.zeros(st_v.shape[1:], jnp.float32)

    def forward_step(t, carry):
        c, j = t // n_vt, t % n_vt
        prev = jnp.maximum(t - 1, 0)
        for jj in range(n_vt):
            @pl.when(t == jj)
            def _():
                w_copy(jj).wait()

        @pl.when(t == 0)
        def _():
            own_p.wait_recv()

        @pl.when(t == n_vt)
        def _():
            x_h0.wait_recv()
            y_h0.wait_recv()
            m1_p.start()
            d_h0.start()
            m1_p.wait_recv()

        @pl.when(t == 2 * n_vt)
        def _():
            x_h1.wait_recv()
            y_h1.wait_recv()
            m2_p.start()
            d_h1.start()
            m2_p.wait_recv()

        @pl.when(t == 3 * n_vt)
        def _():
            d_h0.wait_recv()
            d_h1.wait_recv()
            d_p.start()
            d_p.wait_recv()

        @pl.when(j == 0)
        def _():
            a_copy(c).start()

        @pl.when(t >= n_vt)
        def _():
            z_copy(t - n_vt).wait()

        words = pl.ds(pl.multiple_of(j * VT, VT), VT)
        z_v[j] = lax.dot_general(
            w_v[words, :], a_v[chunk_at(c), :], (((1,), (1,)), ((), ())), preferred_element_type=jnp.float32
        )
        stats_pass(prev // n_vt, prev % n_vt)

        @pl.when(j == n_vt - 1)
        def _():
            low = (vocab_local - PAD_COLS) // 8 * 8 - (n_vt - 1) * VT
            ids = (n_vt - 1) * VT + low + lax.broadcasted_iota(jnp.int32, (VT - low, chunk), 0)
            z_v[j, low:VT, :] = jnp.where(ids < valid, z_v[j, low:VT, :], -jnp.inf)

        @pl.when(t < 3 * n_vt)
        def _():
            z_copy(t).start()

        @pl.when((j == 0) & (t > 0))
        def _():
            send_stats(prev // n_vt)

        return carry

    lax.fori_loop(0, 4 * n_vt, forward_step, 0)
    stats_pass(jnp.int32(3), jnp.int32(n_vt - 1))
    send_stats(jnp.int32(3))

    for copy in (x_h0, y_h0, own_p, x_h1, y_h1, m1_p, m2_p, d_h0, d_h1, d_p):
        copy.wait_send()
    for c in range(4):
        a_copy(c).wait()

    w_row = row_v[1:2, :]
    row_v[3:4, :] = w_row / jnp.sum(w_row)
    for c in range(4):
        for r in range(1, 8):
            st_copy(c, r).wait_recv()
    loss = jnp.zeros((1, LANES), jnp.float32)
    for rel in range(8):
        for h in range(2):
            u = unit_of(rel, h)
            parts = []
            for r in range(8):
                v = unit_of(rel ^ r, h)
                parts.append([st_v[r, i:i + 1, v * LANES:(v + 1) * LANES] for i in range(3)])
            row_max = functools.reduce(jnp.maximum, [p[0] for p in parts])
            row_sum = sum(p[1] * jnp.exp(p[0] - row_max) for p in parts)
            target = sum(p[2] for p in parts)
            log_norm = row_max + jnp.log(row_sum)
            row_v[2:3, u * LANES:(u + 1) * LANES] = log_norm
            loss += row_v[3:4, u * LANES:(u + 1) * LANES] * (log_norm - target)
    loss_ref[...] = jnp.broadcast_to(jnp.sum(loss, axis=1, keepdims=True), loss_ref.shape)

    per_half = n_vt // 2
    half_words = per_half * VT
    word_f = lax.broadcasted_iota(jnp.int32, (LANES, LANES), 0).astype(jnp.float32)

    def dz_pass(c, j, q):
        out_at = (q % 2) * 2 + j
        for lt in range(chunk // LANES):
            cols = slice(lt * LANES, (lt + 1) * LANES)
            log_norm, scale = row_at(2, c, lt), row_at(3, c, lt)
            lab = row_at(0, c, lt) - (j * half_words).astype(jnp.float32) - word_f
            to_a = pl.ds(pl.multiple_of(out_at * chunk + lt * LANES, LANES), LANES)
            for b in range(0, half_words, LANES):
                z = z_v[j * per_half + b // VT, b % VT:b % VT + LANES, cols]
                hit = jnp.where(lab == float(b), 1.0, 0.0)
                d = ((jnp.exp(z - log_norm) - hit) * scale).astype(jnp.bfloat16)
                a_v[b:b + LANES, to_a] = d
                to_dz = pl.ds(pl.multiple_of(j * half_words + b, LANES), LANES)
                dz_v[q % 2, cols, to_dz] = jnp.transpose(d)

    def dz_copy(q, j):
        out_at = (q % 2) * 2 + j
        src = a_v.at[0:half_words, pl.ds(pl.multiple_of(out_at * chunk, chunk), chunk)]
        dst = dz_out.at[pl.ds(pl.multiple_of(j * half_words, half_words), half_words), chunk_at(3 - q)]
        return pltpu.make_async_copy(src, dst, dz_sem.at[out_at])

    def z_reload(s):
        j = s % 2
        src = z_hbm.at[pl.ds((2 - s // 2) * n_vt + j * per_half, per_half)]
        return pltpu.make_async_copy(src, z_v.at[pl.ds(j * per_half, per_half)], z_sem.at[j])

    def first_dz(j, carry):
        dz_pass(jnp.int32(3), j, jnp.int32(0))
        dz_copy(jnp.int32(0), j).start()
        z_reload(j).start()
        return carry

    lax.fori_loop(0, 2, first_dz, 0)

    def prt_copy(s):
        slot = s % 2
        return remote(out_v.at[slot, mine:chunk], prt_v.at[slot], prt_send.at[slot], prt_recv.at[slot], 1)

    d_x = remote(dsend_v.at[0], drecv_v.at[0], d_send.at[0], d_recv.at[0], 2)
    d_y = remote(dsend_v.at[1], drecv_v.at[1], d_send.at[1], d_recv.at[1], 4)

    def stage_copy(s, out, first_out, count):
        j = s % 2
        return pltpu.make_async_copy(
            stage_v.at[j, 0:count],
            out.at[pl.ds(first_out, count), pl.ds(pl.multiple_of(j * NT, NT), NT)],
            stage_sem.at[j],
        )

    def combine(s):
        slot = s % 2
        prt_copy(s).wait_recv()

        @pl.when(s < 2)
        def _():
            dsend_v[slot] = out_v[slot, 0:mine, :] + prt_v[slot]

        @pl.when(s == 0)
        def _():
            d_x.start()

        @pl.when(s == 1)
        def _():
            d_y.start()

        @pl.when(s >= 4)
        def _():
            stage_copy(s, px_out, 0, half).wait()

        @pl.when((s >= 2) & (s < 6) & (slot == 0))
        def _():
            first = pl.multiple_of((2 - s // 2) * half, half)
            stage_v[0, 0:half, :] = out_v[0, 0:half, :] + prt_v[0, 0:half, :]
            hold_v[0, pl.ds(first, half), :] = out_v[0, half:mine, :] + prt_v[0, half:mine, :]
            stage_copy(s, px_out, first, half).start()

        @pl.when((s >= 2) & (s < 6) & (slot == 1))
        def _():
            first = pl.multiple_of((2 - s // 2) * half, half)
            stage_v[1, 0:half, :] = out_v[1, half:mine, :] + prt_v[1, half:mine, :]
            hold_v[1, pl.ds(first, half), :] = out_v[1, 0:half, :] + prt_v[1, 0:half, :]
            stage_copy(s, py_out, first, half).start()

        @pl.when(s >= 6)
        def _():
            stage_v[slot] = out_v[slot, 0:mine, :] + prt_v[slot]
            stage_copy(s, pown_out, 0, mine).start()

        @pl.when(s < 6)
        def _():
            pl.semaphore_signal(credit, inc=1, device_id={"vp": peers[1]}, device_id_type=MESH)

    def backward_step(s, carry):
        q, j = s // 2, s % 2
        slot = s % 2

        @pl.when((s >= 1) & (s < 5))
        def _():
            z_reload(s + 1).start()

        @pl.when(s < 6)
        def _():
            z_reload(s).wait()

        @pl.when(s >= 2)
        def _():
            dz_copy(q - 1, j).wait()
            prt_copy(s).wait_send()

        cols = pl.ds(pl.multiple_of(j * NT, NT), NT)
        out_v[slot] = jnp.dot(dz_v[q % 2], w_v[:, cols], preferred_element_type=jnp.float32)
        dz_pass(jnp.maximum(2 - q, 0), j, q + 1)

        @pl.when(q < 3)
        def _():
            dz_copy(q + 1, j).start()

        @pl.when(s >= 1)
        def _():
            combine(s - 1)

        @pl.when(s >= 2)
        def _():
            pl.semaphore_wait(credit, 1)

        prt_copy(s).start()
        return carry

    lax.fori_loop(0, 8, backward_step, 0)
    combine(jnp.int32(7))

    d_x.wait_recv()
    hold_v[0] += drecv_v[0]
    fin_y = pltpu.make_async_copy(hold_v.at[0], py_out.at[:, 0:NT], fin_sem.at[0])
    fin_y.start()
    d_y.wait_recv()
    hold_v[1] += drecv_v[1]
    fin_x = pltpu.make_async_copy(hold_v.at[1], px_out.at[:, NT:2 * NT], fin_sem.at[1])
    fin_x.start()

    for copy in (*metas, d_x, d_y):
        copy.wait_send()
    for c in range(4):
        for r in range(1, 8):
            st_copy(c, r).wait_send()
    for s in (6, 7):
        prt_copy(s).wait_send()
        stage_copy(s, pown_out, 0, mine).wait()
        dz_copy(3, s % 2).wait()
    fin_y.wait()
    fin_x.wait()


def head(hidden, labels, loss_weight, norm_gain, w_t):
    tok_dev, width = hidden.shape
    tokens = 8 * tok_dev
    vocab_local = w_t.shape[0]
    padded = -(-vocab_local // VT) * VT
    chunk = 2 * tok_dev
    n_vt = padded // VT
    meta = jnp.concatenate(
        [labels.astype(jnp.float32)[None], loss_weight[None], jnp.zeros((6, tok_dev), jnp.float32)], axis=0
    )
    f32, bf16 = jnp.float32, jnp.bfloat16
    hbm = pl.BlockSpec(memory_space=pltpu.MemorySpace.HBM)
    whole = pl.BlockSpec(memory_space=pltpu.VMEM)
    dma = pltpu.SemaphoreType.DMA
    return pl.pallas_call(
        head_kernel,
        out_shape=[
            jax.ShapeDtypeStruct((tokens, width), bf16),
            jax.ShapeDtypeStruct((padded, tokens), bf16),
            jax.ShapeDtypeStruct((tok_dev, width), f32),
            jax.ShapeDtypeStruct((tok_dev, width), f32),
            jax.ShapeDtypeStruct((tok_dev, width), f32),
            jax.ShapeDtypeStruct((3 * n_vt, VT, chunk), f32),
            jax.ShapeDtypeStruct((8, LANES), f32),
        ],
        in_specs=[hbm, whole, whole, hbm],
        out_specs=[hbm] * 6 + [whole],
        scratch_shapes=[
            pltpu.VMEM((padded, width), bf16),
            pltpu.VMEM((tokens, width), bf16),
            pltpu.VMEM((n_vt, VT, chunk), f32),
            pltpu.VMEM((2, chunk, padded), bf16),
            pltpu.VMEM((8, 8, tok_dev), f32),
            pltpu.VMEM((8, tokens), f32),
            pltpu.VMEM((8, chunk), f32),
            pltpu.VMEM((8, chunk), f32),
            pltpu.VMEM((8, chunk), f32),
            pltpu.VMEM((8, 8, tokens), f32),
            pltpu.VMEM((2, chunk, NT), f32),
            pltpu.VMEM((2, tok_dev, NT), f32),
            pltpu.VMEM((2, tok_dev, NT), f32),
            pltpu.VMEM((2, tok_dev, NT), f32),
            pltpu.VMEM((2, tok_dev, NT), f32),
            pltpu.VMEM((2, tok_dev, NT), f32),
            dma((10,)), dma((10,)), dma((7,)), dma((7,)), dma((28,)), dma((28,)),
            dma((2,)), dma((2,)), dma((2,)), dma((2,)),
            dma, dma((n_vt,)), dma((n_vt,)), dma((4,)), dma((4,)), dma((2,)), dma((2,)),
            pltpu.SemaphoreType.REGULAR,
        ],
        compiler_params=pltpu.CompilerParams(
            collective_id=0, has_side_effects=True, vmem_limit_bytes=VMEM_BYTES
        ),
        cost_estimate=pl.CostEstimate(
            flops=4 * tokens * width * padded, bytes_accessed=120_000_000, transcendentals=2 * tokens * padded
        ),
        name="head",
    )(hidden, meta, norm_gain[None], w_t)


def tail_kernel(hidden_ref, gain_ref, own_ref, x_ref, y_ref, dh_ref, dgain_ref, buf, send, recv):
    me = lax.axis_index("vp")
    peers = xor_peers(me)
    barrier = pltpu.get_barrier_semaphore()
    for r in range(1, 8):
        pl.semaphore_signal(barrier, inc=1, device_id={"vp": peers[r]}, device_id_type=MESH)
    rows, width = hidden_ref.shape
    acc = jnp.zeros((8, width), jnp.float32)
    for b in range(0, rows, 32):
        at = slice(b, b + 32)
        x = hidden_ref[at, :].astype(jnp.float32)
        inv_rms = lax.rsqrt(jnp.mean(x * x, axis=-1, keepdims=True) + NORM_EPS)
        n = x * inv_rms
        g = own_ref[at, :] + x_ref[at, :] + y_ref[at, :]
        gn = g * n
        for i in range(0, 32, 8):
            acc += gn[i:i + 8, :]
        u = g * gain_ref[...]
        dh_ref[at, :] = (inv_rms * (u - n * jnp.mean(u * n, axis=-1, keepdims=True))).astype(jnp.bfloat16)
    buf[0] = jnp.sum(acc, axis=0, keepdims=True)
    pl.semaphore_wait(barrier, 7)
    copies = [
        pltpu.make_async_remote_copy(
            src_ref=buf.at[0], dst_ref=buf.at[r], send_sem=send.at[r - 1], recv_sem=recv.at[r - 1],
            device_id={"vp": peers[r]}, device_id_type=MESH,
        )
        for r in range(1, 8)
    ]
    for copy in copies:
        copy.start()
    for copy in copies:
        copy.wait()
    pairs = [buf[2 * r] + buf[2 * r + 1] for r in range(4)]
    dgain_ref[...] = (pairs[0] + pairs[1]) + (pairs[2] + pairs[3])


def tail(hidden, norm_gain, own, from_x, from_y):
    tok_dev, width = hidden.shape
    whole = pl.BlockSpec(memory_space=pltpu.VMEM)
    return pl.pallas_call(
        tail_kernel,
        out_shape=[
            jax.ShapeDtypeStruct((tok_dev, width), jnp.bfloat16),
            jax.ShapeDtypeStruct((1, width), jnp.float32),
        ],
        in_specs=[whole] * 5,
        out_specs=[whole] * 2,
        scratch_shapes=[
            pltpu.VMEM((8, 1, width), jnp.float32),
            pltpu.SemaphoreType.DMA((7,)),
            pltpu.SemaphoreType.DMA((7,)),
        ],
        compiler_params=pltpu.CompilerParams(collective_id=1, has_side_effects=True),
        cost_estimate=pl.CostEstimate(flops=10 * tok_dev * width, bytes_accessed=8_000_000, transcendentals=0),
        name="tail",
    )(hidden, norm_gain[None], own, from_x, from_y)


def weight_grad_kernel(dz_ref, a_ref, out_ref):
    out_ref[...] = jnp.dot(dz_ref[...], a_ref[...], preferred_element_type=jnp.float32)


def weight_grad(dz_t, a_all, vocab_local):
    tokens, width = a_all.shape
    padded = dz_t.shape[0]
    return pl.pallas_call(
        weight_grad_kernel,
        grid=(padded // VT, width // NT),
        out_shape=jax.ShapeDtypeStruct((vocab_local, width), jnp.float32),
        in_specs=[pl.BlockSpec((VT, tokens), lambda i, j: (i, 0)), pl.BlockSpec((tokens, NT), lambda i, j: (0, j))],
        out_specs=pl.BlockSpec((VT, NT), lambda i, j: (i, j)),
        compiler_params=pltpu.CompilerParams(
            vmem_limit_bytes=VMEM_BYTES, dimension_semantics=("arbitrary", "arbitrary")
        ),
        cost_estimate=pl.CostEstimate(
            flops=2 * tokens * width * padded, bytes_accessed=80_000_000, transcendentals=0
        ),
        name="weight_grad",
    )(dz_t, a_all)


def solution(mesh):
    group_size = mesh.shape["vp"]

    def local_step(hidden, labels, loss_weight, norm_gain, w_local):
        vocab_local = w_local.shape[1]
        a_all, dz_t, px, py, pown, _, loss = head(hidden, labels, loss_weight, norm_gain, w_local.T)
        from_x = lax.ppermute(px, "vp", [(i, i ^ 2) for i in range(group_size)])
        from_y = lax.ppermute(py, "vp", [(i, i ^ 4) for i in range(group_size)])
        d_unembed = weight_grad(dz_t, a_all, vocab_local).T
        d_input, d_gain = tail(hidden, norm_gain, pown, from_x, from_y)
        return loss[0, :1], d_input, d_unembed, d_gain[0]

    return jax.shard_map(
        local_step,
        mesh=mesh,
        in_specs=(P(("dp", "vp"), None), P(("dp", "vp")), P(("dp", "vp")), P(None), P(None, "vp")),
        out_specs=(P("dp"), P(("dp", "vp"), None), P("dp", "vp"), P("dp")),
        check_vma=False,
    )
```

```python
import functools

import jax
import jax.numpy as jnp
from jax import lax
from jax.experimental import pallas as pl
from jax.experimental.pallas import tpu as pltpu
from jax.sharding import PartitionSpec as P

NORM_EPS = 1e-5
PAD_COLS = 128
LANES = 128
VT = 1024
NT = 1024
EARLY = 512
LOWEST = -3.0e38
MESH = pl.DeviceIdType.MESH
VMEM_BYTES = 67_000_000


def xor_peers(me):
    step_core = 1 - 2 * (me % 2)
    step_x = 2 - 4 * ((me // 2) % 2)
    step_y = 4 - 8 * (me // 4)
    return [me + (r % 2) * step_core + ((r // 2) % 2) * step_x + (r // 4) * step_y for r in range(8)]


def unit_of(rel, half):
    if rel in (0, 1):
        return 2 * rel + half
    if rel in (6, 7):
        return 12 + 2 * (rel - 6) + half
    return {2: 4, 4: 5, 3: 6, 5: 7}[rel] + 4 * half


def head_kernel(
    hidden_hbm, label_ref, weight_ref, gain_ref, w_hbm,
    a_out, dz_out, px_out, py_out, pown_out, z_hbm, loss_ref,
    w_v, a_v, z_e, z_o, dz_e, dz_o, meta_v, row_v, m_v, s_v, t_v, st_v,
    out_v, prt_v, drecv_v, dsend_v, hold_v, first_v, own_v, erecv_v,
    ag_send, ag_recv, meta_send, meta_recv, st_send, st_recv, prt_send, prt_recv, d_send, d_recv, e_send, e_recv,
    in_sem, w_sem, z_sem, a_sem, dz_sem, put_sem, credit,
):
    me = lax.axis_index("vp")
    peers = xor_peers(me)
    vocab_local, width = w_hbm.shape
    vocab_real = 8 * vocab_local - PAD_COLS
    padded = w_v.shape[0]
    n_vt = padded // VT
    tok_dev = hidden_hbm.shape[0]
    chunk = 2 * tok_dev
    half = tok_dev // 2
    quart = tok_dev // 4
    mine = tok_dev
    z_refs = (z_e, z_o)
    dz_refs = (dz_e, dz_o)

    def remote(src, dst, send, recv, rel):
        return pltpu.make_async_remote_copy(
            src_ref=src, dst_ref=dst, send_sem=send, recv_sem=recv,
            device_id={"vp": peers[rel]}, device_id_type=MESH,
        )

    hidden_v = dz_e.at[0:tok_dev, 0:width]
    hidden_copy = pltpu.make_async_copy(hidden_hbm, hidden_v, in_sem)
    hidden_copy.start()
    barrier = pltpu.get_barrier_semaphore()
    for r in range(1, 8):
        pl.semaphore_signal(barrier, inc=1, device_id={"vp": peers[r]}, device_id_type=MESH)

    def w_copy(j):
        hi = min((j + 1) * VT, vocab_local)
        return pltpu.make_async_copy(w_hbm.at[j * VT:hi], w_v.at[j * VT:hi], w_sem.at[j])

    for j in range(n_vt):
        w_copy(j).start()
    meta_v[0, 0:1, :] = label_ref[...].astype(jnp.float32)
    meta_v[0, 1:2, :] = weight_ref[...]

    hidden_copy.wait()
    for b in range(0, tok_dev, 32):
        x = dz_e[b:b + 32, 0:width].astype(jnp.float32)
        inv_rms = lax.rsqrt(jnp.mean(x * x, axis=-1, keepdims=True) + NORM_EPS)
        a_v[b:b + 32, :] = (x * inv_rms * gain_ref[...]).astype(jnp.bfloat16)
    pl.semaphore_wait(barrier, 7)

    def ag(idx, src, dst, count, rel):
        return remote(
            a_v.at[src:src + count], a_v.at[dst:dst + count], ag_send.at[idx], ag_recv.at[idx], rel
        )

    c1, c2, c3 = chunk, 2 * chunk, 3 * chunk
    own_p = ag(0, 0, mine, mine, 1)
    x_h0 = ag(1, 0, c1, half, 2)
    y_h0 = ag(2, 0, c1 + half, half, 4)
    m1_p = ag(3, c1, c1 + mine, mine, 1)
    x_h1 = ag(4, half, c2, half, 2)
    y_h1 = ag(5, half, c2 + half, half, 4)
    m2_p = ag(6, c2, c2 + mine, mine, 1)
    d_x0 = ag(7, c1 + half, c3, quart, 2)
    d_y0 = ag(8, c1 + quart, c3 + quart, quart, 4)
    d_x1 = ag(9, c2 + half, c3 + half, quart, 2)
    d_y1 = ag(10, c2 + quart, c3 + half + quart, quart, 4)
    d_p = ag(11, c3, c3 + mine, mine, 1)
    metas = [remote(meta_v.at[0], meta_v.at[r], meta_send.at[r - 1], meta_recv.at[r - 1], r) for r in range(1, 8)]
    own_p.start()
    for copy in (*metas, x_h0, y_h0, x_h1, y_h1):
        copy.start()
    w_v[vocab_local:padded, :] = jnp.zeros((padded - vocab_local, width), jnp.bfloat16)
    st_v[0] = jnp.zeros(st_v.shape[1:], jnp.float32)

    base_f = (me * vocab_local).astype(jnp.float32)
    valid = jnp.minimum(vocab_local, vocab_real - me * vocab_local)

    def chunk_at(c):
        return pl.ds(pl.multiple_of(c * chunk, chunk), chunk)

    def row_at(row, c, lt):
        return row_v[row:row + 1, pl.ds(pl.multiple_of(c * chunk + lt * LANES, LANES), LANES)]

    def a_copy(c):
        return pltpu.make_async_copy(a_v.at[chunk_at(c)], a_out.at[chunk_at(c)], a_sem.at[c])

    def z_copy(c, j):
        return pltpu.make_async_copy(z_refs[j % 2].at[j // 2], z_hbm.at[c * n_vt + j], z_sem.at[j])

    group = 256
    sub_f = lax.broadcasted_iota(jnp.int32, (8, LANES), 0).astype(jnp.float32)
    step_f = 8.0 * lax.broadcasted_iota(jnp.int32, (group // 8, 8, LANES), 0).astype(jnp.float32)

    def stats_pass(c, j):
        for lt in range(chunk // LANES):
            cols = slice(lt * LANES, (lt + 1) * LANES)
            lab = row_at(0, c, lt) - float(j * VT) - sub_f
            if j == 0:
                m = jnp.full((8, LANES), LOWEST, jnp.float32)
                s = t = jnp.zeros((8, LANES), jnp.float32)
            else:
                m, s, t = m_v[:, cols], s_v[:, cols], t_v[:, cols]
            for b in range(0, VT, group):
                z = z_refs[j % 2][j // 2, b:b + group, cols].reshape(group // 8, 8, LANES)
                m_new = jnp.maximum(m, jnp.max(z, axis=0))
                s = s * jnp.exp(m - m_new) + jnp.sum(jnp.exp(z - m_new[None]), axis=0)
                t += jnp.sum(jnp.where((lab - float(b))[None] == step_f, z, 0.0), axis=0)
                m = m_new
            m_v[:, cols] = m
            s_v[:, cols] = s
            t_v[:, cols] = t

    def st_copy(c, r):
        at = (slice(None), chunk_at(c))
        return remote(st_v.at[(0, *at)], st_v.at[(r, *at)], st_send.at[c * 7 + r - 1], st_recv.at[c * 7 + r - 1], r)

    def send_stats(c):
        m = m_v[...]
        m_row = jnp.max(m, axis=0, keepdims=True)
        st_v[0, 0:1, chunk_at(c)] = m_row
        st_v[0, 1:2, chunk_at(c)] = jnp.sum(s_v[...] * jnp.exp(m - m_row), axis=0, keepdims=True)
        st_v[0, 2:3, chunk_at(c)] = jnp.sum(t_v[...], axis=0, keepdims=True)
        for r in range(1, 8):
            st_copy(c, r).start()

    def logits(c, j, first, count):
        tokens = pl.ds(pl.multiple_of(c * chunk + first, mine), count)
        z_refs[j % 2][j // 2, :, first:first + count] = lax.dot_general(
            w_v[j * VT:(j + 1) * VT, :], a_v[tokens, :], (((1,), (1,)), ((), ())),
            preferred_element_type=jnp.float32,
        )

    def forward_chunk(c, carry):
        @pl.when(c == 0)
        def _():
            w_copy(0).wait()
            w_copy(1).wait()

        @pl.when(c == 1)
        def _():
            x_h0.wait_recv()
            y_h0.wait_recv()
            m1_p.start()
            d_x0.start()
            d_y0.start()

        @pl.when(c == 2)
        def _():
            x_h1.wait_recv()
            y_h1.wait_recv()
            m2_p.start()
            d_x1.start()
            d_y1.start()

        @pl.when(c == 3)
        def _():
            for copy in (d_x0, d_y0, d_x1, d_y1):
                copy.wait_recv()
            d_p.start()

        before = jnp.maximum(c - 1, 0)

        @pl.when(c > 0)
        def _():
            z_copy(before, 0).wait()
            z_copy(before, 1).wait()

        logits(c, 0, 0, mine)
        stats_pass(before, 3)

        @pl.when(c > 0)
        def _():
            send_stats(before)

        logits(c, 1, 0, mine)

        @pl.when(c == 0)
        def _():
            for copy in metas:
                copy.wait_recv()
            for rel in range(8):
                for h in range(2):
                    u = unit_of(rel, h)
                    row_v[:, u * LANES:(u + 1) * LANES] = meta_v[rel, :, h * LANES:(h + 1) * LANES]
            local = row_v[0:1, :] - base_f
            row_v[0:1, :] = jnp.where(local < float(vocab_local), local, -1.0)
            own_p.wait_recv()

        for cc, copy in ((1, m1_p), (2, m2_p), (3, d_p)):
            @pl.when(c == cc)
            def _():
                copy.wait_recv()

        a_copy(c).start()
        logits(c, 0, mine, mine)

        @pl.when(c < 3)
        def _():
            z_copy(c, 0).start()

        logits(c, 1, mine, mine)
        stats_pass(c, 0)

        @pl.when(c < 3)
        def _():
            z_copy(c, 1).start()

        for j in range(2, n_vt):
            @pl.when(c == 0)
            def _():
                w_copy(j).wait()

            @pl.when(c > 0)
            def _():
                z_copy(before, j).wait()

            logits(c, j, 0, chunk)
            stats_pass(c, j - 1)
            if j == n_vt - 1:
                low = (vocab_local - PAD_COLS) // 8 * 8 - j * VT
                ids = j * VT + low + lax.broadcasted_iota(jnp.int32, (VT - low, chunk), 0)
                last = z_refs[j % 2]
                last[j // 2, low:VT, :] = jnp.where(ids < valid, last[j // 2, low:VT, :], -jnp.inf)

            @pl.when(c < 3)
            def _():
                z_copy(c, j).start()

        return carry

    lax.fori_loop(0, 4, forward_chunk, 0)
    stats_pass(3, 3)
    send_stats(3)

    for copy in (x_h0, y_h0, own_p, x_h1, y_h1, m1_p, m2_p, d_x0, d_y0, d_x1, d_y1, d_p):
        copy.wait_send()
    for c in range(4):
        a_copy(c).wait()

    w_row = row_v[1:2, :]
    row_v[3:4, :] = w_row / jnp.sum(w_row)
    for c in range(4):
        for r in range(1, 8):
            st_copy(c, r).wait_recv()
    loss = jnp.zeros((1, LANES), jnp.float32)
    for rel in range(8):
        for h in range(2):
            u = unit_of(rel, h)
            parts = []
            for r in range(8):
                v = unit_of(rel ^ r, h)
                parts.append([st_v[r, i:i + 1, v * LANES:(v + 1) * LANES] for i in range(3)])
            row_max = functools.reduce(jnp.maximum, [p[0] for p in parts])
            row_sum = sum(p[1] * jnp.exp(p[0] - row_max) for p in parts)
            target = sum(p[2] for p in parts)
            log_norm = row_max + jnp.log(row_sum)
            row_v[2:3, u * LANES:(u + 1) * LANES] = log_norm
            loss += row_v[3:4, u * LANES:(u + 1) * LANES] * (log_norm - target)
    loss_ref[...] = jnp.broadcast_to(jnp.sum(loss, axis=1, keepdims=True), loss_ref.shape)

    half_words = 2 * VT
    word_f = lax.broadcasted_iota(jnp.int32, (LANES, LANES), 0).astype(jnp.float32)

    def dz_pass(c, j, parity):
        out_at = parity * 2 + j
        for lt in range(chunk // LANES):
            cols = slice(lt * LANES, (lt + 1) * LANES)
            log_norm, scale = row_at(2, c, lt), row_at(3, c, lt)
            lab = row_at(0, c, lt) - (j * half_words).astype(jnp.float32) - word_f
            to_a = pl.ds(pl.multiple_of(out_at * chunk + lt * LANES, LANES), LANES)
            for b in range(0, half_words, LANES):
                z = z_refs[b // VT][j, b % VT:b % VT + LANES, cols]
                hit = jnp.where(lab == float(b), 1.0, 0.0)
                d = ((jnp.exp(z - log_norm) - hit) * scale).astype(jnp.bfloat16)
                a_v[b:b + LANES, to_a] = d
                to_dz = pl.ds(pl.multiple_of(j * half_words + b, LANES), LANES)
                dz_refs[parity][cols, to_dz] = jnp.transpose(d)

    def dz_copy(c, j, parity):
        out_at = parity * 2 + j
        src = a_v.at[0:half_words, pl.ds(pl.multiple_of(out_at * chunk, chunk), chunk)]
        dst = dz_out.at[pl.ds(pl.multiple_of(j * half_words, half_words), half_words), chunk_at(c)]
        return pltpu.make_async_copy(src, dst, dz_sem.at[out_at])

    def z_reload(c, j):
        return [
            pltpu.make_async_copy(z_hbm.at[c * n_vt + 2 * j + i], z_refs[i].at[j], z_sem.at[2 * j + i])
            for i in range(2)
        ]

    def first_dz(j, carry):
        dz_pass(3, j, 0)
        for copy in z_reload(2, j):
            copy.start()
        return carry

    lax.fori_loop(0, 2, first_dz, 0)

    def prt_copy(slot):
        return remote(out_v.at[slot, mine:chunk], prt_v.at[slot], prt_send.at[slot], prt_recv.at[slot], 1)

    def d_copy(route, j):
        return remote(
            dsend_v.at[j, route * half:(route + 1) * half], drecv_v.at[route, j],
            d_send.at[route * 2 + j], d_recv.at[route * 2 + j], 2 << route,
        )

    def e_copy(route):
        return remote(first_v.at[route, 0, :, 0:EARLY], erecv_v.at[route], e_send.at[route], e_recv.at[route], 2 << route)

    outs = (px_out, py_out)

    def put_first(route, j):
        skip = EARLY if j == 0 else 0
        return pltpu.make_async_copy(
            first_v.at[route, j, :, skip:NT], outs[route].at[:, j * NT + skip - EARLY:(j + 1) * NT - EARLY],
            put_sem.at[route * 2 + j],
        )

    def put_hold(route, j):
        at = width - EARLY + j * NT
        return pltpu.make_async_copy(
            hold_v.at[route, j], outs[route].at[:, at:at + NT], put_sem.at[4 + route * 2 + j]
        )

    def put_own(j):
        return pltpu.make_async_copy(own_v.at[j], pown_out.at[:, j * NT:(j + 1) * NT], put_sem.at[8 + j])

    def combine(s):
        slot = s % 2
        prt_copy(slot).wait_recv()
        for q in range(4):
            for j in range(2):
                @pl.when(s == 2 * q + j)
                def _():
                    if q == 0:
                        dsend_v[j] = out_v[j, 0:mine, :] + prt_v[j]
                        d_copy(0, j).start()
                        d_copy(1, j).start()
                    elif q == 3:
                        own_v[j] = out_v[j, 0:mine, :] + prt_v[j]
                    else:
                        hold_at, first_at = ((0, half), (half, 0))[q - 1]
                        hold_to, first_to = ((0, 1), (1, 0))[q - 1]
                        hold_v[hold_to, j] = out_v[j, hold_at:hold_at + half, :] + prt_v[j, hold_at:hold_at + half, :]
                        first_v[first_to, j] = (
                            out_v[j, first_at:first_at + half, :] + prt_v[j, first_at:first_at + half, :]
                        )
                        if j == 0:
                            e_copy(first_to).start()
                        put_first(first_to, j).start()

        @pl.when(s < 6)
        def _():
            pl.semaphore_signal(credit, inc=1, device_id={"vp": peers[1]}, device_id_type=MESH)

    def backward_step(q, j, parity):
        s = 2 * q + j
        after = jnp.maximum(2 - q, 0)

        @pl.when((q >= 1) & (q < 3))
        def _():
            for copy in z_reload(after, j):
                copy.wait()

        @pl.when(q == 0)
        def _():
            for copy in z_reload(2, j):
                copy.wait()
            dz_copy(3, j, 0).start()

        @pl.when(q >= 1)
        def _():
            dz_copy(4 - q, j, 1 - parity).wait()
            prt_copy(j).wait_send()

        cols = pl.ds(pl.multiple_of(j * NT, NT), NT)
        out_v[j] = jnp.dot(dz_refs[parity][...], w_v[:, cols], preferred_element_type=jnp.float32)
        dz_pass(after, j, 1 - parity)

        @pl.when(q < 2)
        def _():
            for copy in z_reload(1 - q, j):
                copy.start()

        @pl.when(q < 3)
        def _():
            dz_copy(2 - q, j, 1 - parity).start()

        @pl.when(s >= 1)
        def _():
            combine(s - 1)

        @pl.when(s >= 2)
        def _():
            pl.semaphore_wait(credit, 1)

        prt_copy(j).start()

    def backward_pair(qq, carry):
        for parity in range(2):
            def step(j, inner):
                backward_step(2 * qq + parity, j, parity)
                return inner
            lax.fori_loop(0, 2, step, 0)
        return carry

    lax.fori_loop(0, 2, backward_pair, 0)
    combine(jnp.int32(7))

    for j in range(2):
        for route in range(2):
            d_copy(route, j).wait_recv()
            hold_v[1 - route, j] += drecv_v[route, j]
            put_hold(1 - route, j).start()
    put_own(1).start()
    for route in range(2):
        e_copy(route).wait_recv()
        own_v[0, route * half:(route + 1) * half, 0:EARLY] += erecv_v[route]
    put_own(0).start()

    for copy in metas:
        copy.wait_send()
    for c in range(4):
        for r in range(1, 8):
            st_copy(c, r).wait_send()
    for j in range(2):
        prt_copy(j).wait_send()
        dz_copy(0, j, 1).wait()
        put_own(j).wait()
        e_copy(j).wait_send()
        for route in range(2):
            d_copy(route, j).wait_send()
            put_first(route, j).wait()
            put_hold(route, j).wait()


def head(hidden, labels, loss_weight, norm_gain, w_t):
    tok_dev, width = hidden.shape
    tokens = 8 * tok_dev
    vocab_local = w_t.shape[0]
    padded = -(-vocab_local // VT) * VT
    chunk = 2 * tok_dev
    n_vt = padded // VT
    half = tok_dev // 2
    f32, bf16 = jnp.float32, jnp.bfloat16
    hbm = pl.BlockSpec(memory_space=pltpu.MemorySpace.HBM)
    whole = pl.BlockSpec(memory_space=pltpu.VMEM)
    dma = pltpu.SemaphoreType.DMA
    return pl.pallas_call(
        head_kernel,
        out_shape=[
            jax.ShapeDtypeStruct((tokens, width), bf16),
            jax.ShapeDtypeStruct((padded, tokens), bf16),
            jax.ShapeDtypeStruct((half, 2 * width - EARLY), f32),
            jax.ShapeDtypeStruct((half, 2 * width - EARLY), f32),
            jax.ShapeDtypeStruct((tok_dev, width), f32),
            jax.ShapeDtypeStruct((3 * n_vt, VT, chunk), f32),
            jax.ShapeDtypeStruct((8, LANES), f32),
        ],
        in_specs=[hbm, whole, whole, whole, hbm],
        out_specs=[hbm] * 6 + [whole],
        scratch_shapes=[
            pltpu.VMEM((padded, width), bf16),
            pltpu.VMEM((tokens, width), bf16),
            pltpu.VMEM((n_vt // 2, VT, chunk), f32),
            pltpu.VMEM((n_vt // 2, VT, chunk), f32),
            pltpu.VMEM((chunk, padded), bf16),
            pltpu.VMEM((chunk, padded), bf16),
            pltpu.VMEM((8, 8, tok_dev), f32),
            pltpu.VMEM((8, tokens), f32),
            pltpu.VMEM((8, chunk), f32),
            pltpu.VMEM((8, chunk), f32),
            pltpu.VMEM((8, chunk), f32),
            pltpu.VMEM((8, 8, tokens), f32),
            pltpu.VMEM((2, chunk, NT), f32),
            pltpu.VMEM((2, tok_dev, NT), f32),
            pltpu.VMEM((2, 2, half, NT), f32),
            pltpu.VMEM((2, tok_dev, NT), f32),
            pltpu.VMEM((2, 2, half, NT), f32),
            pltpu.VMEM((2, 2, half, NT), f32),
            pltpu.VMEM((2, tok_dev, NT), f32),
            pltpu.VMEM((2, half, EARLY), f32),
            dma((12,)), dma((12,)), dma((7,)), dma((7,)), dma((28,)), dma((28,)),
            dma((2,)), dma((2,)), dma((4,)), dma((4,)), dma((2,)), dma((2,)),
            dma, dma((n_vt,)), dma((n_vt,)), dma((4,)), dma((4,)), dma((10,)),
            pltpu.SemaphoreType.REGULAR,
        ],
        compiler_params=pltpu.CompilerParams(
            collective_id=0, has_side_effects=True, vmem_limit_bytes=VMEM_BYTES
        ),
        cost_estimate=pl.CostEstimate(
            flops=4 * tokens * width * padded, bytes_accessed=120_000_000, transcendentals=2 * tokens * padded
        ),
        name="head",
    )(hidden, labels[None], loss_weight[None], norm_gain[None], w_t)


def tail_kernel(hidden_ref, gain_ref, own_ref, x_ref, y_ref, dh_ref, dgain_ref, buf, send, recv):
    me = lax.axis_index("vp")
    peers = xor_peers(me)
    barrier = pltpu.get_barrier_semaphore()
    for r in range(1, 8):
        pl.semaphore_signal(barrier, inc=1, device_id={"vp": peers[r]}, device_id_type=MESH)
    rows, width = hidden_ref.shape
    half = rows // 2
    early = 2 * width - x_ref.shape[1]
    acc = jnp.zeros((8, width), jnp.float32)
    for b in range(0, rows, 32):
        at = slice(b, b + 32)
        x = hidden_ref[at, :].astype(jnp.float32)
        inv_rms = lax.rsqrt(jnp.mean(x * x, axis=-1, keepdims=True) + NORM_EPS)
        n = x * inv_rms
        part, rest = (x_ref, y_ref) if b < half else (y_ref, x_ref)
        here = slice(b % half, b % half + 32)
        own = own_ref[at, :] + rest[here, width - early:]
        g = jnp.concatenate([own[:, :early], own[:, early:] + part[here, 0:width - early]], axis=1)
        gn = g * n
        for i in range(0, 32, 8):
            acc += gn[i:i + 8, :]
        u = g * gain_ref[...]
        dh_ref[at, :] = (inv_rms * (u - n * jnp.mean(u * n, axis=-1, keepdims=True))).astype(jnp.bfloat16)
    buf[0] = jnp.sum(acc, axis=0, keepdims=True)
    pl.semaphore_wait(barrier, 7)
    copies = [
        pltpu.make_async_remote_copy(
            src_ref=buf.at[0], dst_ref=buf.at[r], send_sem=send.at[r - 1], recv_sem=recv.at[r - 1],
            device_id={"vp": peers[r]}, device_id_type=MESH,
        )
        for r in range(1, 8)
    ]
    for copy in copies:
        copy.start()
    for copy in copies:
        copy.wait()
    pairs = [buf[2 * r] + buf[2 * r + 1] for r in range(4)]
    dgain_ref[...] = (pairs[0] + pairs[1]) + (pairs[2] + pairs[3])


def tail(hidden, norm_gain, own, from_x, from_y):
    tok_dev, width = hidden.shape
    whole = pl.BlockSpec(memory_space=pltpu.VMEM)
    return pl.pallas_call(
        tail_kernel,
        out_shape=[
            jax.ShapeDtypeStruct((tok_dev, width), jnp.bfloat16),
            jax.ShapeDtypeStruct((1, width), jnp.float32),
        ],
        in_specs=[whole] * 5,
        out_specs=[whole] * 2,
        scratch_shapes=[
            pltpu.VMEM((8, 1, width), jnp.float32),
            pltpu.SemaphoreType.DMA((7,)),
            pltpu.SemaphoreType.DMA((7,)),
        ],
        compiler_params=pltpu.CompilerParams(collective_id=1, has_side_effects=True),
        cost_estimate=pl.CostEstimate(flops=10 * tok_dev * width, bytes_accessed=8_000_000, transcendentals=0),
        name="tail",
    )(hidden, norm_gain[None], own, from_x, from_y)


def weight_grad_kernel(dz_ref, a_ref, out_ref):
    out_ref[...] = jnp.dot(dz_ref[...], a_ref[...], preferred_element_type=jnp.float32)


def weight_grad(dz_t, a_all, vocab_local):
    tokens, width = a_all.shape
    padded = dz_t.shape[0]
    return pl.pallas_call(
        weight_grad_kernel,
        grid=(padded // VT, width // NT),
        out_shape=jax.ShapeDtypeStruct((vocab_local, width), jnp.float32),
        in_specs=[pl.BlockSpec((VT, tokens), lambda i, j: (i, 0)), pl.BlockSpec((tokens, NT), lambda i, j: (0, j))],
        out_specs=pl.BlockSpec((VT, NT), lambda i, j: (i, j)),
        compiler_params=pltpu.CompilerParams(
            vmem_limit_bytes=VMEM_BYTES, dimension_semantics=("arbitrary", "arbitrary")
        ),
        cost_estimate=pl.CostEstimate(
            flops=2 * tokens * width * padded, bytes_accessed=80_000_000, transcendentals=0
        ),
        name="weight_grad",
    )(dz_t, a_all)


def solution(mesh):
    group_size = mesh.shape["vp"]

    def local_step(hidden, labels, loss_weight, norm_gain, w_local):
        vocab_local = w_local.shape[1]
        a_all, dz_t, px, py, pown, _, loss = head(hidden, labels, loss_weight, norm_gain, w_local.T)
        from_x = lax.ppermute(px, "vp", [(i, i ^ 2) for i in range(group_size)])
        from_y = lax.ppermute(py, "vp", [(i, i ^ 4) for i in range(group_size)])
        d_unembed = weight_grad(dz_t, a_all, vocab_local).T
        d_input, d_gain = tail(hidden, norm_gain, pown, from_x, from_y)
        return loss[0, :1], d_input, d_unembed, d_gain[0]

    return jax.shard_map(
        local_step,
        mesh=mesh,
        in_specs=(P(("dp", "vp"), None), P(("dp", "vp")), P(("dp", "vp")), P(None), P(None, "vp")),
        out_specs=(P("dp"), P(("dp", "vp"), None), P("dp", "vp"), P("dp")),
        check_vma=False,
    )
```

```python
import functools

import jax
import jax.numpy as jnp
from jax import lax
from jax.experimental import pallas as pl
from jax.experimental.pallas import tpu as pltpu
from jax.sharding import PartitionSpec as P

NORM_EPS = 1e-5
PAD_COLS = 128
LANES = 128
VT = 1024
NT = 1024
GROUP = 256
EARLY = 512
MESH = pl.DeviceIdType.MESH
VMEM_BYTES = 67_000_000


def xor_peers(me):
    step_core = 1 - 2 * (me % 2)
    step_x = 2 - 4 * ((me // 2) % 2)
    step_y = 4 - 8 * (me // 4)
    return [me + (r % 2) * step_core + ((r // 2) % 2) * step_x + (r // 4) * step_y for r in range(8)]


def unit_of(rel, half):
    if rel in (0, 1):
        return 2 * rel + half
    if rel in (6, 7):
        return 12 + 2 * (rel - 6) + half
    return {2: 4, 4: 5, 3: 6, 5: 7}[rel] + 4 * half


def head_kernel(
    hidden_hbm, label_ref, weight_ref, gain_ref, w_hbm,
    a_out, dz_out, px_out, py_out, pown_out, z_hbm, loss_ref,
    w_v, a_v, z_e, z_o, dz_e, dz_o, meta_v, row_v, m_v, s_v, t_v, st_v,
    out_v, prt_v, drecv_v, dsend_v, hold_v, first_v, own_v, erecv_v,
    ag_send, ag_recv, meta_send, meta_recv, st_send, st_recv, prt_send, prt_recv, d_send, d_recv, e_send, e_recv,
    in_sem, w_sem, z_sem, a_sem, dz_sem, put_sem, credit,
):
    me = lax.axis_index("vp")
    peers = xor_peers(me)
    vocab_local, width = w_hbm.shape
    vocab_real = 8 * vocab_local - PAD_COLS
    padded = w_v.shape[0]
    n_vt = padded // VT
    tok_dev = hidden_hbm.shape[0]
    chunk = 2 * tok_dev
    half = tok_dev // 2
    quart = tok_dev // 4
    mine = tok_dev
    z_refs = (z_e, z_o)
    dz_refs = (dz_e, dz_o)

    def remote(src, dst, send, recv, rel):
        return pltpu.make_async_remote_copy(
            src_ref=src, dst_ref=dst, send_sem=send, recv_sem=recv,
            device_id={"vp": peers[rel]}, device_id_type=MESH,
        )

    hidden_v = dz_e.at[0:tok_dev, 0:width]
    hidden_copy = pltpu.make_async_copy(hidden_hbm, hidden_v, in_sem)
    hidden_copy.start()
    barrier = pltpu.get_barrier_semaphore()
    for r in range(1, 8):
        pl.semaphore_signal(barrier, inc=1, device_id={"vp": peers[r]}, device_id_type=MESH)

    def w_copy(j):
        hi = min((j + 1) * VT, vocab_local)
        return pltpu.make_async_copy(w_hbm.at[j * VT:hi], w_v.at[j * VT:hi], w_sem.at[j])

    for j in range(n_vt):
        w_copy(j).start()
    meta_v[0, 0:1, :] = label_ref[...].astype(jnp.float32)
    meta_v[0, 1:2, :] = weight_ref[...]

    hidden_copy.wait()
    for b in range(0, tok_dev, 32):
        x = dz_e[b:b + 32, 0:width].astype(jnp.float32)
        inv_rms = lax.rsqrt(jnp.mean(x * x, axis=-1, keepdims=True) + NORM_EPS)
        a_v[b:b + 32, :] = (x * inv_rms * gain_ref[...]).astype(jnp.bfloat16)
    pl.semaphore_wait(barrier, 7)

    def ag(idx, src, dst, count, rel):
        return remote(
            a_v.at[src:src + count], a_v.at[dst:dst + count], ag_send.at[idx], ag_recv.at[idx], rel
        )

    c1, c2, c3 = chunk, 2 * chunk, 3 * chunk
    own_p = ag(0, 0, mine, mine, 1)
    x_h0 = ag(1, 0, c1, half, 2)
    y_h0 = ag(2, 0, c1 + half, half, 4)
    m1_p = ag(3, c1, c1 + mine, mine, 1)
    x_h1 = ag(4, half, c2, half, 2)
    y_h1 = ag(5, half, c2 + half, half, 4)
    m2_p = ag(6, c2, c2 + mine, mine, 1)
    d_x0 = ag(7, c1 + half, c3, quart, 2)
    d_y0 = ag(8, c1 + quart, c3 + quart, quart, 4)
    d_x1 = ag(9, c2 + half, c3 + half, quart, 2)
    d_y1 = ag(10, c2 + quart, c3 + half + quart, quart, 4)
    d_p = ag(11, c3, c3 + mine, mine, 1)
    metas = [remote(meta_v.at[0], meta_v.at[r], meta_send.at[r - 1], meta_recv.at[r - 1], r) for r in range(1, 8)]
    own_p.start()
    for copy in (*metas, x_h0, y_h0, x_h1, y_h1):
        copy.start()
    w_v[vocab_local:padded, :] = jnp.zeros((padded - vocab_local, width), jnp.bfloat16)
    st_v[0] = jnp.zeros(st_v.shape[1:], jnp.float32)

    base_f = (me * vocab_local).astype(jnp.float32)
    valid = jnp.minimum(vocab_local, vocab_real - me * vocab_local)

    def chunk_at(c):
        return pl.ds(pl.multiple_of(c * chunk, chunk), chunk)

    def row_at(row, c, lt):
        return row_v[row:row + 1, pl.ds(pl.multiple_of(c * chunk + lt * LANES, LANES), LANES)]

    def a_copy(c):
        return pltpu.make_async_copy(a_v.at[chunk_at(c)], a_out.at[chunk_at(c)], a_sem.at[c])

    def z_copy(c, j):
        return pltpu.make_async_copy(z_refs[j % 2].at[j // 2], z_hbm.at[c * n_vt + j], z_sem.at[j])

    sub_f = lax.broadcasted_iota(jnp.int32, (GROUP, LANES), 0).astype(jnp.float32)
    groups = VT // GROUP

    def stats_pass(c, j):
        for lt in range(chunk // LANES):
            cols = slice(lt * LANES, (lt + 1) * LANES)
            lab = row_at(0, c, lt) - float(j * VT) - sub_f
            for b in range(groups):
                z = z_refs[j % 2][j // 2, b * GROUP:(b + 1) * GROUP, cols]
                z3 = z.reshape(GROUP // 8, 8, LANES)
                m = jnp.max(z3, axis=0)
                hit = jnp.where(lab == float(b * GROUP), z, 0.0)
                m_v[j * groups + b, :, cols] = m
                s_v[j * groups + b, :, cols] = jnp.sum(jnp.exp(z3 - m[None]), axis=0)
                t_v[j * groups + b, :, cols] = jnp.sum(hit.reshape(GROUP // 8, 8, LANES), axis=0)

    def st_copy(c, r):
        at = (slice(None), chunk_at(c))
        return remote(st_v.at[(0, *at)], st_v.at[(r, *at)], st_send.at[c * 7 + r - 1], st_recv.at[c * 7 + r - 1], r)

    def send_stats(c):
        m = m_v[...]
        m_row = jnp.max(jnp.max(m, axis=0), axis=0, keepdims=True)
        s_all = jnp.sum(s_v[...] * jnp.exp(m - m_row[None]), axis=0)
        st_v[0, 0:1, chunk_at(c)] = m_row
        st_v[0, 1:2, chunk_at(c)] = jnp.sum(s_all, axis=0, keepdims=True)
        st_v[0, 2:3, chunk_at(c)] = jnp.sum(jnp.sum(t_v[...], axis=0), axis=0, keepdims=True)
        for r in range(1, 8):
            st_copy(c, r).start()

    def logits(c, j, first, count):
        tokens = pl.ds(pl.multiple_of(c * chunk + first, mine), count)
        z_refs[j % 2][j // 2, :, first:first + count] = lax.dot_general(
            w_v[j * VT:(j + 1) * VT, :], a_v[tokens, :], (((1,), (1,)), ((), ())),
            preferred_element_type=jnp.float32,
        )

    def forward_chunk(c, carry):
        @pl.when(c == 0)
        def _():
            w_copy(0).wait()
            w_copy(1).wait()

        @pl.when(c == 1)
        def _():
            x_h0.wait_recv()
            y_h0.wait_recv()
            m1_p.start()
            d_x0.start()
            d_y0.start()

        @pl.when(c == 2)
        def _():
            x_h1.wait_recv()
            y_h1.wait_recv()
            m2_p.start()
            d_x1.start()
            d_y1.start()

        @pl.when(c == 3)
        def _():
            for copy in (d_x0, d_y0, d_x1, d_y1):
                copy.wait_recv()
            d_p.start()

        before = jnp.maximum(c - 1, 0)

        @pl.when(c > 0)
        def _():
            z_copy(before, 0).wait()
            z_copy(before, 1).wait()

        logits(c, 0, 0, mine)
        logits(c, 1, 0, mine)
        stats_pass(before, 3)

        @pl.when(c > 0)
        def _():
            send_stats(before)

        @pl.when(c == 0)
        def _():
            for copy in metas:
                copy.wait_recv()
            for rel in range(8):
                for h in range(2):
                    u = unit_of(rel, h)
                    row_v[:, u * LANES:(u + 1) * LANES] = meta_v[rel, :, h * LANES:(h + 1) * LANES]
            local = row_v[0:1, :] - base_f
            row_v[0:1, :] = jnp.where(local < float(vocab_local), local, -1.0)
            own_p.wait_recv()

        for cc, copy in ((1, m1_p), (2, m2_p), (3, d_p)):
            @pl.when(c == cc)
            def _():
                copy.wait_recv()

        a_copy(c).start()
        logits(c, 0, mine, mine)
        logits(c, 1, mine, mine)

        @pl.when(c < 3)
        def _():
            z_copy(c, 0).start()
            z_copy(c, 1).start()

        for j in range(2, n_vt):
            @pl.when(c == 0)
            def _():
                w_copy(j).wait()

            @pl.when(c > 0)
            def _():
                z_copy(before, j).wait()

            logits(c, j, 0, chunk)
            stats_pass(c, j - 2)
            if j == n_vt - 1:
                stats_pass(c, j - 1)
                low = (vocab_local - PAD_COLS) // 8 * 8 - j * VT
                ids = j * VT + low + lax.broadcasted_iota(jnp.int32, (VT - low, chunk), 0)
                last = z_refs[j % 2]
                last[j // 2, low:VT, :] = jnp.where(ids < valid, last[j // 2, low:VT, :], -jnp.inf)

            @pl.when(c < 3)
            def _():
                z_copy(c, j).start()

        return carry

    lax.fori_loop(0, 4, forward_chunk, 0)
    stats_pass(3, 3)
    send_stats(3)

    for copy in (x_h0, y_h0, own_p, x_h1, y_h1, m1_p, m2_p, d_x0, d_y0, d_x1, d_y1, d_p):
        copy.wait_send()
    for c in range(4):
        a_copy(c).wait()

    w_row = row_v[1:2, :]
    row_v[3:4, :] = w_row / jnp.sum(w_row)
    for c in range(4):
        for r in range(1, 8):
            st_copy(c, r).wait_recv()
    loss = jnp.zeros((1, LANES), jnp.float32)
    for rel in range(8):
        for h in range(2):
            u = unit_of(rel, h)
            parts = []
            for r in range(8):
                v = unit_of(rel ^ r, h)
                parts.append([st_v[r, i:i + 1, v * LANES:(v + 1) * LANES] for i in range(3)])
            row_max = functools.reduce(jnp.maximum, [p[0] for p in parts])
            row_sum = sum(p[1] * jnp.exp(p[0] - row_max) for p in parts)
            target = sum(p[2] for p in parts)
            log_norm = row_max + jnp.log(row_sum)
            row_v[2:3, u * LANES:(u + 1) * LANES] = log_norm
            loss += row_v[3:4, u * LANES:(u + 1) * LANES] * (log_norm - target)
    loss_ref[...] = jnp.broadcast_to(jnp.sum(loss, axis=1, keepdims=True), loss_ref.shape)

    half_words = 2 * VT
    word_f = lax.broadcasted_iota(jnp.int32, (LANES, LANES), 0).astype(jnp.float32)

    def dz_pass(c, j, parity):
        out_at = parity * 2 + j
        for lt in range(chunk // LANES):
            cols = slice(lt * LANES, (lt + 1) * LANES)
            log_norm, scale = row_at(2, c, lt), row_at(3, c, lt)
            lab = row_at(0, c, lt) - (j * half_words).astype(jnp.float32) - word_f
            to_a = pl.ds(pl.multiple_of(out_at * chunk + lt * LANES, LANES), LANES)
            for b in range(0, half_words, LANES):
                z = z_refs[b // VT][j, b % VT:b % VT + LANES, cols]
                hit = jnp.where(lab == float(b), 1.0, 0.0)
                d = ((jnp.exp(z - log_norm) - hit) * scale).astype(jnp.bfloat16)
                a_v[b:b + LANES, to_a] = d
                to_dz = pl.ds(pl.multiple_of(j * half_words + b, LANES), LANES)
                dz_refs[parity][cols, to_dz] = jnp.transpose(d)

    def dz_copy(c, j, parity):
        out_at = parity * 2 + j
        src = a_v.at[0:half_words, pl.ds(pl.multiple_of(out_at * chunk, chunk), chunk)]
        dst = dz_out.at[pl.ds(pl.multiple_of(j * half_words, half_words), half_words), chunk_at(c)]
        return pltpu.make_async_copy(src, dst, dz_sem.at[out_at])

    def z_reload(c, j):
        return [
            pltpu.make_async_copy(z_hbm.at[c * n_vt + 2 * j + i], z_refs[i].at[j], z_sem.at[2 * j + i])
            for i in range(2)
        ]

    def first_dz(j, carry):
        dz_pass(3, j, 0)
        for copy in z_reload(2, j):
            copy.start()
        return carry

    lax.fori_loop(0, 2, first_dz, 0)

    def prt_copy(slot):
        return remote(out_v.at[slot, mine:chunk], prt_v.at[slot], prt_send.at[slot], prt_recv.at[slot], 1)

    def d_copy(route, j):
        return remote(
            dsend_v.at[j, route * half:(route + 1) * half], drecv_v.at[route, j],
            d_send.at[route * 2 + j], d_recv.at[route * 2 + j], 2 << route,
        )

    def e_copy(route):
        return remote(first_v.at[route, 0, :, 0:EARLY], erecv_v.at[route], e_send.at[route], e_recv.at[route], 2 << route)

    outs = (px_out, py_out)

    def put_first(route, j):
        skip = EARLY if j == 0 else 0
        return pltpu.make_async_copy(
            first_v.at[route, j, :, skip:NT], outs[route].at[:, j * NT + skip - EARLY:(j + 1) * NT - EARLY],
            put_sem.at[route * 2 + j],
        )

    def put_hold(route, j):
        at = width - EARLY + j * NT
        return pltpu.make_async_copy(
            hold_v.at[route, j], outs[route].at[:, at:at + NT], put_sem.at[4 + route * 2 + j]
        )

    def put_own(j):
        return pltpu.make_async_copy(own_v.at[j], pown_out.at[:, j * NT:(j + 1) * NT], put_sem.at[8 + j])

    def combine(s):
        slot = s % 2
        prt_copy(slot).wait_recv()
        for q in range(4):
            for j in range(2):
                @pl.when(s == 2 * q + j)
                def _():
                    if q == 0:
                        dsend_v[j] = out_v[j, 0:mine, :] + prt_v[j]
                        d_copy(0, j).start()
                        d_copy(1, j).start()
                    elif q == 3:
                        own_v[j] = out_v[j, 0:mine, :] + prt_v[j]
                    else:
                        hold_at, first_at = ((0, half), (half, 0))[q - 1]
                        hold_to, first_to = ((0, 1), (1, 0))[q - 1]
                        hold_v[hold_to, j] = out_v[j, hold_at:hold_at + half, :] + prt_v[j, hold_at:hold_at + half, :]
                        first_v[first_to, j] = (
                            out_v[j, first_at:first_at + half, :] + prt_v[j, first_at:first_at + half, :]
                        )
                        if j == 0:
                            e_copy(first_to).start()
                        put_first(first_to, j).start()

        @pl.when(s < 6)
        def _():
            pl.semaphore_signal(credit, inc=1, device_id={"vp": peers[1]}, device_id_type=MESH)

    def backward_step(q, j, parity):
        s = 2 * q + j
        after = jnp.maximum(2 - q, 0)

        @pl.when((q >= 1) & (q < 3))
        def _():
            for copy in z_reload(after, j):
                copy.wait()

        @pl.when(q == 0)
        def _():
            for copy in z_reload(2, j):
                copy.wait()
            dz_copy(3, j, 0).start()

        @pl.when(q >= 1)
        def _():
            dz_copy(4 - q, j, 1 - parity).wait()
            prt_copy(j).wait_send()

        cols = pl.ds(pl.multiple_of(j * NT, NT), NT)
        out_v[j] = jnp.dot(dz_refs[parity][...], w_v[:, cols], preferred_element_type=jnp.float32)
        dz_pass(after, j, 1 - parity)

        @pl.when(q < 2)
        def _():
            for copy in z_reload(1 - q, j):
                copy.start()

        @pl.when(q < 3)
        def _():
            dz_copy(2 - q, j, 1 - parity).start()

        @pl.when(s >= 1)
        def _():
            combine(s - 1)

        @pl.when(s >= 2)
        def _():
            pl.semaphore_wait(credit, 1)

        prt_copy(j).start()

    def backward_pair(qq, carry):
        for parity in range(2):
            def step(j, inner):
                backward_step(2 * qq + parity, j, parity)
                return inner
            lax.fori_loop(0, 2, step, 0)
        return carry

    lax.fori_loop(0, 2, backward_pair, 0)
    combine(jnp.int32(7))

    for j in range(2):
        for route in range(2):
            d_copy(route, j).wait_recv()
            hold_v[1 - route, j] += drecv_v[route, j]
            put_hold(1 - route, j).start()
    put_own(1).start()
    for route in range(2):
        e_copy(route).wait_recv()
        own_v[0, route * half:(route + 1) * half, 0:EARLY] += erecv_v[route]
    put_own(0).start()

    for copy in metas:
        copy.wait_send()
    for c in range(4):
        for r in range(1, 8):
            st_copy(c, r).wait_send()
    for j in range(2):
        prt_copy(j).wait_send()
        dz_copy(0, j, 1).wait()
        put_own(j).wait()
        e_copy(j).wait_send()
        for route in range(2):
            d_copy(route, j).wait_send()
            put_first(route, j).wait()
            put_hold(route, j).wait()


def head(hidden, labels, loss_weight, norm_gain, w_t):
    tok_dev, width = hidden.shape
    tokens = 8 * tok_dev
    vocab_local = w_t.shape[0]
    padded = -(-vocab_local // VT) * VT
    chunk = 2 * tok_dev
    n_vt = padded // VT
    half = tok_dev // 2
    f32, bf16 = jnp.float32, jnp.bfloat16
    hbm = pl.BlockSpec(memory_space=pltpu.MemorySpace.HBM)
    whole = pl.BlockSpec(memory_space=pltpu.VMEM)
    dma = pltpu.SemaphoreType.DMA
    return pl.pallas_call(
        head_kernel,
        out_shape=[
            jax.ShapeDtypeStruct((tokens, width), bf16),
            jax.ShapeDtypeStruct((padded, tokens), bf16),
            jax.ShapeDtypeStruct((half, 2 * width - EARLY), f32),
            jax.ShapeDtypeStruct((half, 2 * width - EARLY), f32),
            jax.ShapeDtypeStruct((tok_dev, width), f32),
            jax.ShapeDtypeStruct((3 * n_vt, VT, chunk), f32),
            jax.ShapeDtypeStruct((8, LANES), f32),
        ],
        in_specs=[hbm, whole, whole, whole, hbm],
        out_specs=[hbm] * 6 + [whole],
        scratch_shapes=[
            pltpu.VMEM((padded, width), bf16),
            pltpu.VMEM((tokens, width), bf16),
            pltpu.VMEM((n_vt // 2, VT, chunk), f32),
            pltpu.VMEM((n_vt // 2, VT, chunk), f32),
            pltpu.VMEM((chunk, padded), bf16),
            pltpu.VMEM((chunk, padded), bf16),
            pltpu.VMEM((8, 8, tok_dev), f32),
            pltpu.VMEM((8, tokens), f32),
            pltpu.VMEM((padded // GROUP, 8, chunk), f32),
            pltpu.VMEM((padded // GROUP, 8, chunk), f32),
            pltpu.VMEM((padded // GROUP, 8, chunk), f32),
            pltpu.VMEM((8, 8, tokens), f32),
            pltpu.VMEM((2, chunk, NT), f32),
            pltpu.VMEM((2, tok_dev, NT), f32),
            pltpu.VMEM((2, 2, half, NT), f32),
            pltpu.VMEM((2, tok_dev, NT), f32),
            pltpu.VMEM((2, 2, half, NT), f32),
            pltpu.VMEM((2, 2, half, NT), f32),
            pltpu.VMEM((2, tok_dev, NT), f32),
            pltpu.VMEM((2, half, EARLY), f32),
            dma((12,)), dma((12,)), dma((7,)), dma((7,)), dma((28,)), dma((28,)),
            dma((2,)), dma((2,)), dma((4,)), dma((4,)), dma((2,)), dma((2,)),
            dma, dma((n_vt,)), dma((n_vt,)), dma((4,)), dma((4,)), dma((10,)),
            pltpu.SemaphoreType.REGULAR,
        ],
        compiler_params=pltpu.CompilerParams(
            collective_id=0, has_side_effects=True, vmem_limit_bytes=VMEM_BYTES,
        ),
        cost_estimate=pl.CostEstimate(
            flops=4 * tokens * width * padded, bytes_accessed=120_000_000, transcendentals=2 * tokens * padded
        ),
        name="head",
    )(hidden, labels[None], loss_weight[None], norm_gain[None], w_t)


def tail_kernel(
    hidden_hbm, gain_ref, own_hbm, x_hbm, y_hbm, dh_ref, dgain_ref, h_v, g_v, x_v, y_v, buf, in_sem, send, recv
):
    me = lax.axis_index("vp")
    peers = xor_peers(me)
    barrier = pltpu.get_barrier_semaphore()
    for r in range(1, 8):
        pl.semaphore_signal(barrier, inc=1, device_id={"vp": peers[r]}, device_id_type=MESH)
    rows, width = hidden_hbm.shape
    half = rows // 2
    rest_at = x_hbm.shape[1] - width
    early = width - rest_at
    step = 64

    def loads(k):
        at = slice(k * step, (k + 1) * step)
        here = slice(k * step % half, k * step % half + step)
        x_cols, y_cols = slice(0, rest_at), slice(rest_at, rest_at + width)
        if k * step >= half:
            x_cols, y_cols = y_cols, x_cols
        return [
            pltpu.make_async_copy(hidden_hbm.at[at], h_v.at[at], in_sem.at[k, 0]),
            pltpu.make_async_copy(own_hbm.at[at], g_v.at[at], in_sem.at[k, 1]),
            pltpu.make_async_copy(x_hbm.at[here, x_cols], x_v.at[here, x_cols], in_sem.at[k, 2]),
            pltpu.make_async_copy(y_hbm.at[here, y_cols], y_v.at[here, y_cols], in_sem.at[k, 3]),
        ]

    for k in range(rows // step):
        for copy in loads(k):
            copy.start()
    acc = jnp.zeros((8, width), jnp.float32)
    for b in range(0, rows, 32):
        if b % step == 0:
            for copy in loads(b // step):
                copy.wait()
        at = slice(b, b + 32)
        here = slice(b % half, b % half + 32)
        part, rest = (x_v, y_v) if b < half else (y_v, x_v)
        x = h_v[at, :].astype(jnp.float32)
        inv_rms = lax.rsqrt(jnp.mean(x * x, axis=-1, keepdims=True) + NORM_EPS)
        own = g_v[at, :] + rest[here, rest_at:rest_at + width]
        g = jnp.concatenate([own[:, :early], own[:, early:] + part[here, 0:rest_at]], axis=1)
        g_v[at, :] = g
        gn = g * (x * inv_rms)
        for i in range(0, 32, 8):
            acc += gn[i:i + 8, :]
    buf[0] = jnp.sum(acc, axis=0, keepdims=True)
    pl.semaphore_wait(barrier, 7)
    copies = [
        pltpu.make_async_remote_copy(
            src_ref=buf.at[0], dst_ref=buf.at[r], send_sem=send.at[r - 1], recv_sem=recv.at[r - 1],
            device_id={"vp": peers[r]}, device_id_type=MESH,
        )
        for r in range(1, 8)
    ]
    for copy in copies:
        copy.start()
    for b in range(0, rows, 32):
        at = slice(b, b + 32)
        x = h_v[at, :].astype(jnp.float32)
        inv_rms = lax.rsqrt(jnp.mean(x * x, axis=-1, keepdims=True) + NORM_EPS)
        n = x * inv_rms
        u = g_v[at, :] * gain_ref[...]
        dh_ref[at, :] = (inv_rms * (u - n * jnp.mean(u * n, axis=-1, keepdims=True))).astype(jnp.bfloat16)
    for copy in copies:
        copy.wait()
    pairs = [buf[2 * r] + buf[2 * r + 1] for r in range(4)]
    dgain_ref[...] = (pairs[0] + pairs[1]) + (pairs[2] + pairs[3])


def tail(hidden, norm_gain, own, from_x, from_y):
    tok_dev, width = hidden.shape
    whole = pl.BlockSpec(memory_space=pltpu.VMEM)
    anywhere = pl.BlockSpec(memory_space=pl.ANY)
    return pl.pallas_call(
        tail_kernel,
        out_shape=[
            jax.ShapeDtypeStruct((tok_dev, width), jnp.bfloat16),
            jax.ShapeDtypeStruct((1, width), jnp.float32),
        ],
        in_specs=[anywhere, whole, anywhere, anywhere, anywhere],
        out_specs=[whole] * 2,
        scratch_shapes=[
            pltpu.VMEM((tok_dev, width), jnp.bfloat16),
            pltpu.VMEM((tok_dev, width), jnp.float32),
            pltpu.VMEM(from_x.shape, jnp.float32),
            pltpu.VMEM(from_y.shape, jnp.float32),
            pltpu.VMEM((8, 1, width), jnp.float32),
            pltpu.SemaphoreType.DMA((4, 4)),
            pltpu.SemaphoreType.DMA((7,)),
            pltpu.SemaphoreType.DMA((7,)),
        ],
        compiler_params=pltpu.CompilerParams(collective_id=1, has_side_effects=True),
        cost_estimate=pl.CostEstimate(flops=10 * tok_dev * width, bytes_accessed=8_000_000, transcendentals=0),
        name="tail",
    )(hidden, norm_gain[None], own, from_x, from_y)


def finish_kernel(dh_ref, dgain_ref, loss_ref, dh_out, dgain_out, loss_out):
    dh_out[...] = dh_ref[...]
    dgain_out[...] = dgain_ref[...]
    loss_out[...] = loss_ref[0:1, 0:1]


def finish(dh, dgain, loss):
    whole = pl.BlockSpec(memory_space=pltpu.VMEM)
    return pl.pallas_call(
        finish_kernel,
        out_shape=[
            jax.ShapeDtypeStruct(dh.shape, dh.dtype),
            jax.ShapeDtypeStruct(dgain.shape, dgain.dtype),
            jax.ShapeDtypeStruct((1, 1), loss.dtype),
        ],
        in_specs=[whole] * 3,
        out_specs=[whole] * 3,
        name="finish",
    )(dh, dgain, loss)


def weight_grad_kernel(dz_hbm, a_hbm, out_hbm, dz_v, a_v, out_v, dz_sem, a_sem, out_sem):
    vocab_local = out_hbm.shape[0]
    n_vt = dz_hbm.shape[0] // VT

    def dz_copy(v):
        return pltpu.make_async_copy(
            dz_hbm.at[pl.ds(pl.multiple_of(v * VT, VT), VT)], dz_v.at[v % 2], dz_sem.at[v % 2]
        )

    def a_copy(d):
        return pltpu.make_async_copy(a_hbm.at[:, d * NT:(d + 1) * NT], a_v.at[:, d * NT:(d + 1) * NT], a_sem.at[d])

    def out_copy(v, d, count):
        return pltpu.make_async_copy(
            out_v.at[d, 0:count],
            out_hbm.at[pl.ds(pl.multiple_of(v * VT, VT), count), pl.ds(pl.multiple_of(d * NT, NT), NT)],
            out_sem.at[d],
        )

    last_count = vocab_local - (n_vt - 1) * VT
    dz_copy(0).start()
    a_copy(0).start()
    a_copy(1).start()
    dz_copy(1).start()

    def step(i, carry):
        v, d = i // 2, i % 2

        @pl.when(d == 0)
        def _():
            dz_copy(v).wait()

        for dd in range(2):
            @pl.when(i == dd)
            def _():
                a_copy(dd).wait()

        @pl.when(i >= 2)
        def _():
            out_copy(v - 1, d, VT).wait()

        cols = pl.ds(pl.multiple_of(d * NT, NT), NT)
        out_v[d] = jnp.dot(dz_v[v % 2], a_v[:, cols], preferred_element_type=jnp.float32)

        @pl.when(v < n_vt - 1)
        def _():
            out_copy(v, d, VT).start()

        @pl.when(v == n_vt - 1)
        def _():
            out_copy(v, d, last_count).start()

        @pl.when((d == 1) & (v < n_vt - 2))
        def _():
            dz_copy(v + 2).start()

        return carry

    lax.fori_loop(0, 2 * n_vt, step, 0)
    for d in range(2):
        out_copy(n_vt - 1, d, last_count).wait()


def weight_grad(dz_t, a_all, vocab_local):
    tokens, width = a_all.shape
    padded = dz_t.shape[0]
    hbm = pl.BlockSpec(memory_space=pltpu.MemorySpace.HBM)
    return pl.pallas_call(
        weight_grad_kernel,
        out_shape=jax.ShapeDtypeStruct((vocab_local, width), jnp.float32),
        in_specs=[hbm, hbm],
        out_specs=hbm,
        scratch_shapes=[
            pltpu.VMEM((2, VT, tokens), jnp.bfloat16),
            pltpu.VMEM((tokens, width), jnp.bfloat16),
            pltpu.VMEM((2, VT, NT), jnp.float32),
            pltpu.SemaphoreType.DMA((2,)),
            pltpu.SemaphoreType.DMA((2,)),
            pltpu.SemaphoreType.DMA((2,)),
        ],
        compiler_params=pltpu.CompilerParams(vmem_limit_bytes=VMEM_BYTES),
        cost_estimate=pl.CostEstimate(
            flops=2 * tokens * width * padded, bytes_accessed=60_000_000, transcendentals=0
        ),
        name="weight_grad",
    )(dz_t, a_all)


def solution(mesh):
    group_size = mesh.shape["vp"]

    def local_step(hidden, labels, loss_weight, norm_gain, w_local):
        vocab_local = w_local.shape[1]
        a_all, dz_t, px, py, pown, _, loss = head(hidden, labels, loss_weight, norm_gain, w_local.T)
        from_x = lax.ppermute(px, "vp", [(i, i ^ 2) for i in range(group_size)])
        from_y = lax.ppermute(py, "vp", [(i, i ^ 4) for i in range(group_size)])
        d_unembed = weight_grad(dz_t, a_all, vocab_local).T
        d_input, d_gain = tail(hidden, norm_gain, pown, from_x, from_y)
        d_input, d_gain, mean_loss = finish(d_input, d_gain, loss)
        return mean_loss[0], d_input, d_unembed, d_gain[0]

    return jax.shard_map(
        local_step,
        mesh=mesh,
        in_specs=(P(("dp", "vp"), None), P(("dp", "vp")), P(("dp", "vp")), P(None), P(None, "vp")),
        out_specs=(P("dp"), P(("dp", "vp"), None), P("dp", "vp"), P("dp")),
        check_vma=False,
    )
```

```python
import functools

import jax
import jax.numpy as jnp
from jax import lax
from jax.experimental import pallas as pl
from jax.experimental.pallas import tpu as pltpu
from jax.sharding import PartitionSpec as P

NORM_EPS = 1e-5
PAD_COLS = 128
LANES = 128
VT = 1024
NT = 1024
GROUP = 128
EARLY = 512
MESH = pl.DeviceIdType.MESH
VMEM_BYTES = 67_000_000
LOWEST = -3.0e38
OTHERS = range(1, 8)


def xor_peers(me):
    step_core = 1 - 2 * (me % 2)
    step_x = 2 - 4 * ((me // 2) % 2)
    step_y = 4 - 8 * (me // 4)
    return [me + (r % 2) * step_core + ((r // 2) % 2) * step_x + (r // 4) * step_y for r in range(8)]


def unit_of(rel, half):
    if rel in (0, 1):
        return 2 * rel + half
    if rel in (6, 7):
        return 12 + 2 * (rel - 6) + half
    return {2: 4, 4: 5, 3: 6, 5: 7}[rel] + 4 * half


def head_kernel(
    hidden_hbm, label_ref, weight_ref, gain_ref, w_hbm,
    a_out, dz_out, px_out, py_out, pown_out, z_hbm, loss_ref,
    w_v, a_v, z_e, z_o, dz_e, dz_o, meta_v, row_v, m_v, s_v, t_v, st_v,
    out_v, prt_v, drecv_v, dsend_v, hold_v, first_v, erecv_v,
    ag_send, ag_recv, meta_send, meta_recv, st_send, st_recv, prt_send, prt_recv, d_send, d_recv, e_send, e_recv,
    in_sem, w_sem, z_sem, a_sem, dz_sem, put_sem, credit,
):
    me = lax.axis_index("vp")
    peers = xor_peers(me)
    vocab_local, width = w_hbm.shape
    vocab_real = 8 * vocab_local - PAD_COLS
    padded = w_v.shape[0]
    n_vt = padded // VT
    tok_dev = hidden_hbm.shape[0]
    chunk = 2 * tok_dev
    half = tok_dev // 2
    quart = tok_dev // 4
    tokens = 4 * chunk
    mine = tok_dev
    z_refs = (z_e, z_o)
    dz_refs = (dz_e, dz_o)

    def remote(src, dst, send, recv, rel):
        return pltpu.make_async_remote_copy(
            src_ref=src, dst_ref=dst, send_sem=send, recv_sem=recv,
            device_id={"vp": peers[rel]}, device_id_type=MESH,
        )

    hidden_v = dz_e.at[0:tok_dev, 0:width]
    hidden_copy = pltpu.make_async_copy(hidden_hbm, hidden_v, in_sem)
    hidden_copy.start()
    barrier = pltpu.get_barrier_semaphore()
    for r in OTHERS:
        pl.semaphore_signal(barrier, inc=1, device_id={"vp": peers[r]}, device_id_type=MESH)

    def w_copy(j):
        hi = min((j + 1) * VT, vocab_local)
        return pltpu.make_async_copy(w_hbm.at[j * VT:hi], w_v.at[j * VT:hi], w_sem.at[j])

    for j in range(n_vt):
        w_copy(j).start()
    meta_v[0, :, 0:tok_dev] = label_ref[...].astype(jnp.float32)
    meta_v[0, :, tok_dev:chunk] = weight_ref[...]

    hidden_copy.wait()
    for b in range(0, tok_dev, 32):
        x = dz_e[b:b + 32, 0:width].astype(jnp.float32)
        inv_rms = lax.rsqrt(jnp.mean(x * x, axis=-1, keepdims=True) + NORM_EPS)
        a_v[b:b + 32, :] = (x * inv_rms * gain_ref[...]).astype(jnp.bfloat16)
    pl.semaphore_wait(barrier, 7)

    def ag(idx, src, dst, count, rel):
        return remote(
            a_v.at[src:src + count], a_v.at[dst:dst + count], ag_send.at[idx], ag_recv.at[idx], rel
        )

    c1, c2, c3 = chunk, 2 * chunk, 3 * chunk
    own_p = ag(0, 0, mine, mine, 1)
    x_h0 = ag(1, 0, c1, half, 2)
    y_h0 = ag(2, 0, c1 + half, half, 4)
    m1_p = ag(3, c1, c1 + mine, mine, 1)
    x_h1 = ag(4, half, c2, half, 2)
    y_h1 = ag(5, half, c2 + half, half, 4)
    m2_p = ag(6, c2, c2 + mine, mine, 1)
    d_x0 = ag(7, c1 + half, c3, quart, 2)
    d_y0 = ag(8, c1 + quart, c3 + quart, quart, 4)
    d_x1 = ag(9, c2 + half, c3 + half, quart, 2)
    d_y1 = ag(10, c2 + quart, c3 + half + quart, quart, 4)
    d_p = ag(11, c3, c3 + mine, mine, 1)
    metas = [remote(meta_v.at[0], meta_v.at[r], meta_send.at[r - 1], meta_recv.at[r - 1], r) for r in OTHERS]
    own_p.start()
    for copy in (*metas, x_h0, y_h0, x_h1, y_h1):
        copy.start()
    w_v[vocab_local:padded, :] = jnp.zeros((padded - vocab_local, width), jnp.bfloat16)

    base_f = (me * vocab_local).astype(jnp.float32)
    valid = jnp.minimum(vocab_local, vocab_real - me * vocab_local)

    def chunk_at(c):
        return pl.ds(pl.multiple_of(c * chunk, chunk), chunk)

    def row_at(row, c, lt):
        return row_v[row:row + 1, pl.ds(pl.multiple_of(c * chunk + lt * LANES, LANES), LANES)]

    def a_copy(c):
        return pltpu.make_async_copy(a_v.at[chunk_at(c)], a_out.at[chunk_at(c)], a_sem.at[c])

    def z_copy(c, j):
        return pltpu.make_async_copy(z_refs[j % 2].at[j // 2], z_hbm.at[c * n_vt + j], z_sem.at[j])

    groups = VT // GROUP

    def stats_pass(j):
        for lt in range(chunk // LANES):
            cols = slice(lt * LANES, (lt + 1) * LANES)
            for b in range(groups):
                z = z_refs[j % 2][j // 2, b * GROUP:(b + 1) * GROUP, cols].reshape(GROUP // 8, 8, LANES)
                m = jnp.max(z, axis=0)
                m_v[j * groups + b, :, cols] = m
                s_v[j * groups + b, :, cols] = jnp.sum(jnp.exp(z - m[None]), axis=0)

    def st_copy(c, r):
        at = c * 7 + r - 1
        return remote(st_v.at[0, c], st_v.at[r, c], st_send.at[at], st_recv.at[at], r)

    def send_stats(c):
        m = m_v[...]
        m_row = jnp.max(jnp.max(m, axis=0), axis=0, keepdims=True)
        s_all = jnp.sum(s_v[...] * jnp.exp(m - m_row[None]), axis=0)
        st_v[0, c, :, 0:chunk] = m_row
        st_v[0, c, :, chunk:2 * chunk] = jnp.sum(s_all, axis=0, keepdims=True)
        for r in OTHERS:
            st_copy(c, r).start()

    def logits(c, j, first, count):
        tokens = pl.ds(pl.multiple_of(c * chunk + first, mine), count)
        z_refs[j % 2][j // 2, :, first:first + count] = lax.dot_general(
            w_v[j * VT:(j + 1) * VT, :], a_v[tokens, :], (((1,), (1,)), ((), ())),
            preferred_element_type=jnp.float32,
        )

    def forward_chunk(c, carry):
        @pl.when(c == 0)
        def _():
            w_copy(0).wait()
            w_copy(1).wait()

        @pl.when(c == 1)
        def _():
            x_h0.wait_recv()
            y_h0.wait_recv()
            m1_p.start()
            d_x0.start()
            d_y0.start()

        @pl.when(c == 2)
        def _():
            x_h1.wait_recv()
            y_h1.wait_recv()
            m2_p.start()
            d_x1.start()
            d_y1.start()

        @pl.when(c == 3)
        def _():
            for copy in (d_x0, d_y0, d_x1, d_y1):
                copy.wait_recv()
            d_p.start()

        before = jnp.maximum(c - 1, 0)

        @pl.when(c > 0)
        def _():
            z_copy(before, 0).wait()
            z_copy(before, 1).wait()

        logits(c, 0, 0, mine)
        logits(c, 1, 0, mine)
        stats_pass(3)

        @pl.when(c > 0)
        def _():
            send_stats(before)

        @pl.when(c == 0)
        def _():
            for copy in metas:
                copy.wait_recv()
            for rel in range(8):
                for h in range(2):
                    u = unit_of(rel, h)
                    for row in range(2):
                        at = row * tok_dev + h * LANES
                        row_v[row:row + 1, u * LANES:(u + 1) * LANES] = meta_v[rel, :, at:at + LANES]
            local = row_v[0:1, :] - base_f
            row_v[0:1, :] = jnp.where(local < float(vocab_local), local, -1.0)
            own_p.wait_recv()

        for cc, copy in ((1, m1_p), (2, m2_p), (3, d_p)):
            @pl.when(c == cc)
            def _():
                copy.wait_recv()

        a_copy(c).start()
        logits(c, 0, mine, mine)
        logits(c, 1, mine, mine)

        @pl.when(c < 3)
        def _():
            z_copy(c, 0).start()
            z_copy(c, 1).start()

        for j in range(2, n_vt):
            @pl.when(c == 0)
            def _():
                w_copy(j).wait()

            @pl.when(c > 0)
            def _():
                z_copy(before, j).wait()

            logits(c, j, 0, chunk)
            stats_pass(j - 2)
            if j == n_vt - 1:
                stats_pass(j - 1)
                low = (vocab_local - PAD_COLS) // 8 * 8 - j * VT
                ids = j * VT + low + lax.broadcasted_iota(jnp.int32, (VT - low, chunk), 0)
                last = z_refs[j % 2]
                last[j // 2, low:VT, :] = jnp.where(ids < valid, last[j // 2, low:VT, :], LOWEST)

            @pl.when(c < 3)
            def _():
                z_copy(c, j).start()

        return carry

    lax.fori_loop(0, 4, forward_chunk, 0)
    stats_pass(3)
    send_stats(3)

    for copy in (x_h0, y_h0, own_p, x_h1, y_h1, m1_p, m2_p, d_x0, d_y0, d_x1, d_y1, d_p):
        copy.wait_send()
    for c in range(4):
        a_copy(c).wait()

    w_row = row_v[1:2, :]
    row_v[3:4, :] = w_row / jnp.sum(w_row)
    for c in range(4):
        for r in OTHERS:
            st_copy(c, r).wait_recv()
    for rel in range(8):
        for h in range(2):
            parts = []
            for r in range(8):
                c, lt = divmod(unit_of(rel ^ r, h), 4)
                parts.append([st_v[r, c, :, at:at + LANES] for at in (lt * LANES, chunk + lt * LANES)])
            row_max = functools.reduce(jnp.maximum, [m for m, _ in parts])
            row_sum = sum(part * jnp.exp(m - row_max) for m, part in parts)
            u = unit_of(rel, h)
            row_v[2:3, u * LANES:(u + 1) * LANES] = row_max + jnp.log(row_sum)

    half_words = 2 * VT
    word_f = lax.broadcasted_iota(jnp.int32, (LANES, LANES), 0).astype(jnp.float32)

    def dz_pass(c, j, parity):
        out_at = parity * 2 + j
        for lt in range(chunk // LANES):
            cols = slice(lt * LANES, (lt + 1) * LANES)
            log_norm, scale = row_at(2, c, lt), row_at(3, c, lt)
            lab = row_at(0, c, lt) - (j * half_words).astype(jnp.float32) - word_f
            to_a = pl.ds(pl.multiple_of(out_at * chunk + lt * LANES, LANES), LANES)
            target = jnp.zeros((8, LANES), jnp.float32)
            for b in range(0, half_words, LANES):
                z = z_refs[b // VT][j, b % VT:b % VT + LANES, cols]
                hit = lab == float(b)
                target += jnp.sum(jnp.where(hit, z, 0.0).reshape(LANES // 8, 8, LANES), axis=0)
                d = ((jnp.exp(z - log_norm) - jnp.where(hit, 1.0, 0.0)) * scale).astype(jnp.bfloat16)
                a_v[b:b + LANES, to_a] = d
                to_dz = pl.ds(pl.multiple_of(j * half_words + b, LANES), LANES)
                dz_refs[parity][cols, to_dz] = jnp.transpose(d)
            t_v[c, j, :, cols] = target

    def dz_copy(c, j, parity):
        out_at = parity * 2 + j
        src = a_v.at[0:half_words, pl.ds(pl.multiple_of(out_at * chunk, chunk), chunk)]
        dst = dz_out.at[pl.ds(pl.multiple_of(j * half_words, half_words), half_words), chunk_at(c)]
        return pltpu.make_async_copy(src, dst, dz_sem.at[out_at])

    def z_reload(c, j):
        return [
            pltpu.make_async_copy(z_hbm.at[c * n_vt + 2 * j + i], z_refs[i].at[j], z_sem.at[2 * j + i])
            for i in range(2)
        ]

    def first_dz(j, carry):
        dz_pass(3, j, 0)
        for copy in z_reload(2, j):
            copy.start()
        return carry

    lax.fori_loop(0, 2, first_dz, 0)

    def prt_copy(slot):
        return remote(out_v.at[slot, mine:chunk], prt_v.at[slot], prt_send.at[slot], prt_recv.at[slot], 1)

    def d_copy(route, j):
        return remote(
            dsend_v.at[j, route * half:(route + 1) * half], drecv_v.at[route, j],
            d_send.at[route * 2 + j], d_recv.at[route * 2 + j], 2 << route,
        )

    def e_copy(route):
        return remote(first_v.at[route, 0, :, 0:EARLY], erecv_v.at[route], e_send.at[route], e_recv.at[route], 2 << route)

    outs = (px_out, py_out)

    def put_first(route, j):
        skip = EARLY if j == 0 else 0
        return pltpu.make_async_copy(
            first_v.at[route, j, :, skip:NT], outs[route].at[:, j * NT + skip - EARLY:(j + 1) * NT - EARLY],
            put_sem.at[route * 2 + j],
        )

    def put_hold(route, j):
        at = width - EARLY + j * NT
        return pltpu.make_async_copy(
            hold_v.at[route, j], outs[route].at[:, at:at + NT], put_sem.at[4 + route * 2 + j]
        )

    def put_own(j):
        return pltpu.make_async_copy(
            out_v.at[j, 0:mine], pown_out.at[:, j * NT:(j + 1) * NT], put_sem.at[8 + j]
        )

    def combine(s):
        slot = s % 2
        prt_copy(slot).wait_recv()
        for q in range(4):
            for j in range(2):
                @pl.when(s == 2 * q + j)
                def _():
                    if q == 0:
                        dsend_v[j] = out_v[j, 0:mine, :] + prt_v[j]
                        d_copy(0, j).start()
                        d_copy(1, j).start()
                    elif q == 3:
                        out_v[j, 0:mine, :] += prt_v[j]
                    else:
                        hold_at, first_at = ((0, half), (half, 0))[q - 1]
                        hold_to, first_to = ((0, 1), (1, 0))[q - 1]
                        hold_v[hold_to, j] = out_v[j, hold_at:hold_at + half, :] + prt_v[j, hold_at:hold_at + half, :]
                        first_v[first_to, j] = (
                            out_v[j, first_at:first_at + half, :] + prt_v[j, first_at:first_at + half, :]
                        )
                        if j == 0:
                            e_copy(first_to).start()
                        put_first(first_to, j).start()

        @pl.when(s < 6)
        def _():
            pl.semaphore_signal(credit, inc=1, device_id={"vp": peers[1]}, device_id_type=MESH)

    def backward_step(q, j, parity):
        s = 2 * q + j
        after = jnp.maximum(2 - q, 0)

        @pl.when((q >= 1) & (q < 3))
        def _():
            for copy in z_reload(after, j):
                copy.wait()

        @pl.when(q == 0)
        def _():
            for copy in z_reload(2, j):
                copy.wait()
            dz_copy(3, j, 0).start()

        @pl.when(q >= 1)
        def _():
            dz_copy(4 - q, j, 1 - parity).wait()
            prt_copy(j).wait_send()

        cols = pl.ds(pl.multiple_of(j * NT, NT), NT)
        out_v[j] = jnp.dot(dz_refs[parity][...], w_v[:, cols], preferred_element_type=jnp.float32)
        dz_pass(after, j, 1 - parity)

        @pl.when(q < 2)
        def _():
            for copy in z_reload(1 - q, j):
                copy.start()

        @pl.when(q < 3)
        def _():
            dz_copy(2 - q, j, 1 - parity).start()

        @pl.when(s >= 1)
        def _():
            combine(s - 1)

        @pl.when(s >= 2)
        def _():
            pl.semaphore_wait(credit, 1)

        prt_copy(j).start()

    def backward_pair(qq, carry):
        for parity in range(2):
            def step(j, inner):
                backward_step(2 * qq + parity, j, parity)
                return inner
            lax.fori_loop(0, 2, step, 0)
        return carry

    lax.fori_loop(0, 2, backward_pair, 0)
    combine(jnp.int32(7))

    loss = jnp.zeros((1, LANES), jnp.float32)
    for u in range(tokens // LANES):
        cols = slice(u * LANES, (u + 1) * LANES)
        c, lt = divmod(u, 4)
        targets = jnp.sum(t_v[c, 0, :, lt * LANES:(lt + 1) * LANES] + t_v[c, 1, :, lt * LANES:(lt + 1) * LANES],
                          axis=0, keepdims=True)
        own_norm = row_v[2:3, cols] if u < tok_dev // LANES else 0.0
        loss += row_v[3:4, cols] * (own_norm - targets)
    loss_ref[...] = loss

    for j in range(2):
        for route in range(2):
            d_copy(route, j).wait_recv()
            hold_v[1 - route, j] += drecv_v[route, j]
            put_hold(1 - route, j).start()
    put_own(1).start()
    for route in range(2):
        e_copy(route).wait_recv()
        out_v[0, route * half:(route + 1) * half, 0:EARLY] += erecv_v[route]
    put_own(0).start()

    for copy in metas:
        copy.wait_send()
    for c in range(4):
        for r in OTHERS:
            st_copy(c, r).wait_send()
    for j in range(2):
        prt_copy(j).wait_send()
        dz_copy(0, j, 1).wait()
        put_own(j).wait()
        e_copy(j).wait_send()
        for route in range(2):
            d_copy(route, j).wait_send()
            put_first(route, j).wait()
            put_hold(route, j).wait()


def head(hidden, labels, loss_weight, norm_gain, w_t):
    tok_dev, width = hidden.shape
    tokens = 8 * tok_dev
    vocab_local = w_t.shape[0]
    padded = -(-vocab_local // VT) * VT
    chunk = 2 * tok_dev
    n_vt = padded // VT
    half = tok_dev // 2
    f32, bf16 = jnp.float32, jnp.bfloat16
    hbm = pl.BlockSpec(memory_space=pltpu.MemorySpace.HBM)
    whole = pl.BlockSpec(memory_space=pltpu.VMEM)
    dma = pltpu.SemaphoreType.DMA
    return pl.pallas_call(
        head_kernel,
        out_shape=[
            jax.ShapeDtypeStruct((tokens, width), bf16),
            jax.ShapeDtypeStruct((padded, tokens), bf16),
            jax.ShapeDtypeStruct((half, 2 * width - EARLY), f32),
            jax.ShapeDtypeStruct((half, 2 * width - EARLY), f32),
            jax.ShapeDtypeStruct((tok_dev, width), f32),
            jax.ShapeDtypeStruct((3 * n_vt, VT, chunk), f32),
            jax.ShapeDtypeStruct((1, LANES), f32),
        ],
        in_specs=[hbm, whole, whole, whole, hbm],
        out_specs=[hbm] * 6 + [whole],
        scratch_shapes=[
            pltpu.VMEM((padded, width), bf16),
            pltpu.VMEM((tokens, width), bf16),
            *[pltpu.VMEM((n_vt // 2, VT, chunk), f32) for _ in "eo"],
            *[pltpu.VMEM((chunk, padded), bf16) for _ in "eo"],
            pltpu.VMEM((8, 1, chunk), f32),
            pltpu.VMEM((8, tokens), f32),
            *[pltpu.VMEM((padded // GROUP, 8, chunk), f32) for _ in "ms"],
            pltpu.VMEM((4, 2, 8, chunk), f32),
            pltpu.VMEM((8, 4, 1, 2 * chunk), f32),
            pltpu.VMEM((2, chunk, NT), f32),
            pltpu.VMEM((2, tok_dev, NT), f32),
            pltpu.VMEM((2, 2, half, NT), f32),
            pltpu.VMEM((2, tok_dev, NT), f32),
            *[pltpu.VMEM((2, 2, half, NT), f32) for _ in "hf"],
            pltpu.VMEM((2, half, EARLY), f32),
            *[dma((count,)) for count in (12, 7, 28, 2, 4, 2) for _ in "sr"],
            dma, dma((n_vt,)), dma((n_vt,)), dma((4,)), dma((4,)), dma((10,)),
            pltpu.SemaphoreType.REGULAR,
        ],
        compiler_params=pltpu.CompilerParams(
            collective_id=0, has_side_effects=True, vmem_limit_bytes=VMEM_BYTES,
        ),
        cost_estimate=pl.CostEstimate(
            flops=4 * tokens * width * padded, bytes_accessed=120_000_000, transcendentals=2 * tokens * padded
        ),
        name="head",
    )(hidden, labels[None], loss_weight[None], norm_gain[None], w_t)


def tail_kernel(
    hidden_hbm, gain_ref, own_hbm, x_hbm, y_hbm, loss_ref, dh_ref, dgain_ref, total_ref, h_v, g_v, x_v, y_v, buf, in_sem, send, recv
):
    me = lax.axis_index("vp")
    peers = xor_peers(me)
    barrier = pltpu.get_barrier_semaphore()
    for r in OTHERS:
        pl.semaphore_signal(barrier, inc=1, device_id={"vp": peers[r]}, device_id_type=MESH)
    rows, width = hidden_hbm.shape
    half = rows // 2
    rest_at = x_hbm.shape[1] - width
    early = width - rest_at
    step = 64

    def loads(k):
        at = slice(k * step, (k + 1) * step)
        here = slice(k * step % half, k * step % half + step)
        x_cols, y_cols = slice(0, rest_at), slice(rest_at, rest_at + width)
        if k * step >= half:
            x_cols, y_cols = y_cols, x_cols
        return [
            pltpu.make_async_copy(hidden_hbm.at[at], h_v.at[at], in_sem.at[k, 0]),
            pltpu.make_async_copy(own_hbm.at[at], g_v.at[at], in_sem.at[k, 1]),
            pltpu.make_async_copy(x_hbm.at[here, x_cols], x_v.at[here, x_cols], in_sem.at[k, 2]),
            pltpu.make_async_copy(y_hbm.at[here, y_cols], y_v.at[here, y_cols], in_sem.at[k, 3]),
        ]

    for k in range(rows // step):
        for copy in loads(k):
            copy.start()
    acc = jnp.zeros((8, width), jnp.float32)
    for b in range(0, rows, 32):
        if b % step == 0:
            for copy in loads(b // step):
                copy.wait()
        at = slice(b, b + 32)
        here = slice(b % half, b % half + 32)
        part, rest = (x_v, y_v) if b < half else (y_v, x_v)
        x = h_v[at, :].astype(jnp.float32)
        inv_rms = lax.rsqrt(jnp.mean(x * x, axis=-1, keepdims=True) + NORM_EPS)
        own = g_v[at, :] + rest[here, rest_at:rest_at + width]
        g = jnp.concatenate([own[:, :early], own[:, early:] + part[here, 0:rest_at]], axis=1)
        g_v[at, :] = g
        gn = g * (x * inv_rms)
        for i in range(0, 32, 8):
            acc += gn[i:i + 8, :]
    buf[0, :, 0:width] = jnp.sum(acc, axis=0, keepdims=True)
    buf[0, :, width:width + LANES] = loss_ref[...]
    pl.semaphore_wait(barrier, 7)
    copies = [
        pltpu.make_async_remote_copy(
            src_ref=buf.at[0], dst_ref=buf.at[r], send_sem=send.at[r - 1], recv_sem=recv.at[r - 1],
            device_id={"vp": peers[r]}, device_id_type=MESH,
        )
        for r in OTHERS
    ]
    for copy in copies:
        copy.start()
    for b in range(0, rows, 32):
        at = slice(b, b + 32)
        x = h_v[at, :].astype(jnp.float32)
        inv_rms = lax.rsqrt(jnp.mean(x * x, axis=-1, keepdims=True) + NORM_EPS)
        n = x * inv_rms
        u = g_v[at, :] * gain_ref[...]
        dh_ref[at, :] = (inv_rms * (u - n * jnp.mean(u * n, axis=-1, keepdims=True))).astype(jnp.bfloat16)
    for copy in copies:
        copy.wait()
    pairs = [buf[2 * r] + buf[2 * r + 1] for r in range(4)]
    total = (pairs[0] + pairs[1]) + (pairs[2] + pairs[3])
    dgain_ref[...] = total[:, 0:width]
    total_ref[...] = jnp.broadcast_to(jnp.sum(total[:, width:], axis=1, keepdims=True), total_ref.shape)


def tail(hidden, norm_gain, own, from_x, from_y, loss):
    tok_dev, width = hidden.shape
    whole = pl.BlockSpec(memory_space=pltpu.VMEM)
    hbm = pl.BlockSpec(memory_space=pltpu.MemorySpace.HBM)
    return pl.pallas_call(
        tail_kernel,
        out_shape=[
            jax.ShapeDtypeStruct((tok_dev, width), jnp.bfloat16),
            jax.ShapeDtypeStruct((1, width), jnp.float32),
            jax.ShapeDtypeStruct((1, LANES), jnp.float32),
        ],
        in_specs=[hbm, whole, hbm, hbm, hbm, whole],
        out_specs=[whole] * 3,
        scratch_shapes=[
            pltpu.VMEM((tok_dev, width), jnp.bfloat16),
            pltpu.VMEM((tok_dev, width), jnp.float32),
            pltpu.VMEM(from_x.shape, jnp.float32),
            pltpu.VMEM(from_y.shape, jnp.float32),
            pltpu.VMEM((8, 1, width + LANES), jnp.float32),
            pltpu.SemaphoreType.DMA((4, 4)),
            *[pltpu.SemaphoreType.DMA((7,)) for _ in "sr"],
        ],
        compiler_params=pltpu.CompilerParams(collective_id=1, has_side_effects=True),
        cost_estimate=pl.CostEstimate(flops=10 * tok_dev * width, bytes_accessed=8_000_000, transcendentals=0),
        name="tail",
    )(hidden, norm_gain[None], own, from_x, from_y, loss)


def finish_kernel(dh_ref, dgain_ref, loss_ref, dh_out, dgain_out, loss_out):
    dh_out[...] = dh_ref[...]
    dgain_out[...] = dgain_ref[...]
    loss_out[...] = loss_ref[:, 0:1]


def finish(dh, dgain, loss):
    whole = pl.BlockSpec(memory_space=pltpu.VMEM)
    return pl.pallas_call(
        finish_kernel,
        out_shape=[
            jax.ShapeDtypeStruct(dh.shape, dh.dtype),
            jax.ShapeDtypeStruct(dgain.shape, dgain.dtype),
            jax.ShapeDtypeStruct((1, 1), loss.dtype),
        ],
        in_specs=[whole] * 3,
        out_specs=[whole] * 3,
        name="finish",
    )(dh, dgain, loss)


def weight_grad_kernel(dz_hbm, a_hbm, out_hbm, dz_v, a_v, out_v, dz_sem, a_sem, out_sem):
    vocab_local = out_hbm.shape[0]
    n_vt = dz_hbm.shape[0] // VT

    def dz_copy(v):
        return pltpu.make_async_copy(
            dz_hbm.at[pl.ds(pl.multiple_of(v * VT, VT), VT)], dz_v.at[v % 2], dz_sem.at[v % 2]
        )

    def a_copy(d):
        return pltpu.make_async_copy(a_hbm.at[:, d * NT:(d + 1) * NT], a_v.at[:, d * NT:(d + 1) * NT], a_sem.at[d])

    def out_copy(v, d, count):
        return pltpu.make_async_copy(
            out_v.at[d, 0:count],
            out_hbm.at[pl.ds(pl.multiple_of(v * VT, VT), count), pl.ds(pl.multiple_of(d * NT, NT), NT)],
            out_sem.at[d],
        )

    last_count = vocab_local - (n_vt - 1) * VT
    dz_copy(0).start()
    a_copy(0).start()
    a_copy(1).start()
    dz_copy(1).start()

    def step(i, carry):
        v, d = i // 2, i % 2

        @pl.when(d == 0)
        def _():
            dz_copy(v).wait()

        for dd in range(2):
            @pl.when(i == dd)
            def _():
                a_copy(dd).wait()

        @pl.when(i >= 2)
        def _():
            out_copy(v - 1, d, VT).wait()

        cols = pl.ds(pl.multiple_of(d * NT, NT), NT)
        out_v[d] = jnp.dot(dz_v[v % 2], a_v[:, cols], preferred_element_type=jnp.float32)

        @pl.when(v < n_vt - 1)
        def _():
            out_copy(v, d, VT).start()

        @pl.when(v == n_vt - 1)
        def _():
            out_copy(v, d, last_count).start()

        @pl.when((d == 1) & (v < n_vt - 2))
        def _():
            dz_copy(v + 2).start()

        return carry

    lax.fori_loop(0, 2 * n_vt, step, 0)
    for d in range(2):
        out_copy(n_vt - 1, d, last_count).wait()


def weight_grad(dz_t, a_all, vocab_local):
    tokens, width = a_all.shape
    padded = dz_t.shape[0]
    hbm = pl.BlockSpec(memory_space=pltpu.MemorySpace.HBM)
    return pl.pallas_call(
        weight_grad_kernel,
        out_shape=jax.ShapeDtypeStruct((vocab_local, width), jnp.float32),
        in_specs=[hbm, hbm],
        out_specs=hbm,
        scratch_shapes=[
            pltpu.VMEM((2, VT, tokens), jnp.bfloat16),
            pltpu.VMEM((tokens, width), jnp.bfloat16),
            pltpu.VMEM((2, VT, NT), jnp.float32),
            *[pltpu.SemaphoreType.DMA((2,)) for _ in "dao"],
        ],
        compiler_params=pltpu.CompilerParams(vmem_limit_bytes=VMEM_BYTES),
        cost_estimate=pl.CostEstimate(
            flops=2 * tokens * width * padded, bytes_accessed=60_000_000, transcendentals=0
        ),
        name="weight_grad",
    )(dz_t, a_all)


def solution(mesh):
    group_size = mesh.shape["vp"]

    def local_step(hidden, labels, loss_weight, norm_gain, w_local):
        vocab_local = w_local.shape[1]
        a_all, dz_t, px, py, pown, _, loss = head(hidden, labels, loss_weight, norm_gain, w_local.T)
        from_x = lax.ppermute(px, "vp", [(i, i ^ 2) for i in range(group_size)])
        from_y = lax.ppermute(py, "vp", [(i, i ^ 4) for i in range(group_size)])
        d_unembed = weight_grad(dz_t, a_all, vocab_local).T
        small = tail(hidden, norm_gain, pown, from_x, from_y, loss)
        d_input, d_gain, mean_loss = finish(*small)
        return mean_loss[0], d_input, d_unembed, d_gain[0]

    return jax.shard_map(
        local_step,
        mesh=mesh,
        in_specs=(P(("dp", "vp"), None), P(("dp", "vp")), P(("dp", "vp")), P(None), P(None, "vp")),
        out_specs=(P("dp"), P(("dp", "vp"), None), P("dp", "vp"), P("dp")),
        check_vma=False,
    )
```

```python
import functools

import jax
import jax.numpy as jnp
from jax import lax
from jax.experimental import pallas as pl
from jax.experimental.pallas import tpu as pltpu
from jax.sharding import PartitionSpec as P

NORM_EPS = 1e-5
PAD_COLS = 128
LANES = 128
VT = 1024
NT = 1024
EARLY = 512
GROUP = 128
MESH = pl.DeviceIdType.MESH
VMEM_BYTES = 67_043_328
LOWEST = -3.0e38
SUBLANES = 8
RELS = range(8)
OTHERS = RELS[1:]


def xor_peers(me):
    step_core = 1 - 2 * (me % 2)
    step_x = 2 - 4 * ((me // 2) % 2)
    step_y = 4 - 8 * (me // 4)
    return [me + (r % 2) * step_core + ((r // 2) % 2) * step_x + (r // 4) * step_y for r in RELS]


def unit_of(rel, half):
    if rel in (0, 1):
        return 2 * rel + half
    if rel in (6, 7):
        return 12 + 2 * (rel - 6) + half
    return {2: 4, 4: 5, 3: 6, 5: 7}[rel] + 4 * half


def head_kernel(
    hidden_hbm, label_hbm, weight_hbm, gain_hbm, w_hbm,
    a_out, dz_out, px_out, py_out, pown_out, z_hbm, loss_out,
    label_v, weight_v, gain_v, loss_v, w_v, a_v, z_e, z_o, dz_e, dz_o, meta_v, row_v, stat_v, t_v, st_v,
    out_v, prt_v, drecv_v, dsend_v, hold_v, first_v,
    ag_send, ag_recv, meta_send, meta_recv, st_send, st_recv, prt_send, prt_recv, d_send, d_recv, e_send, e_recv,
    in_sem, w_sem, z_sem, a_sem, dz_sem, put_sem, credit,
):
    me = lax.axis_index("vp")
    peers = xor_peers(me)
    vocab_local, width = w_hbm.shape
    vocab_real = 8 * vocab_local - PAD_COLS
    padded = w_v.shape[0]
    n_vt = padded // VT
    tok_dev = hidden_hbm.shape[0]
    chunk = 2 * tok_dev
    half = tok_dev // 2
    quart = tok_dev // 4
    tokens = 4 * chunk
    mine = tok_dev
    z_refs = (z_e, z_o)
    dz_refs = (dz_e, dz_o)

    def remote(src, dst, send, recv, rel):
        return pltpu.make_async_remote_copy(
            src_ref=src, dst_ref=dst, send_sem=send, recv_sem=recv,
            device_id={"vp": peers[rel]}, device_id_type=MESH,
        )

    hidden_v = dz_e.at[:tok_dev, :width]
    small = ((hidden_hbm, hidden_v), (label_hbm, label_v), (weight_hbm, weight_v), (gain_hbm, gain_v), (loss_v, loss_out))
    *ins, loss_copy = [pltpu.make_async_copy(src, dst, in_sem.at[i]) for i, (src, dst) in enumerate(small)]
    for copy in ins:
        copy.start()
    barrier = pltpu.get_barrier_semaphore()
    for r in OTHERS:
        pl.semaphore_signal(barrier, inc=1, device_id={"vp": peers[r]}, device_id_type=MESH)

    def w_copy(j):
        hi = min((j + 1) * VT, vocab_local)
        return pltpu.make_async_copy(w_hbm.at[j * VT:hi], w_v.at[j * VT:hi], w_sem.at[j])

    for j in range(n_vt):
        w_copy(j).start()

    for copy in ins:
        copy.wait()
    meta_v[0, :, :tok_dev] = label_v[...].astype(jnp.float32)
    meta_v[0, :, tok_dev:chunk] = weight_v[...]
    for b in range(0, tok_dev, 32):
        x = dz_e[b:b + 32, :width].astype(jnp.float32)
        inv_rms = lax.rsqrt(jnp.mean(x * x, axis=-1, keepdims=True) + NORM_EPS)
        a_v[b:b + 32, :] = (x * inv_rms * gain_v[...]).astype(jnp.bfloat16)
    pl.semaphore_wait(barrier, 7)

    def ag(idx, src, dst, count, rel):
        return remote(
            a_v.at[src:src + count], a_v.at[dst:dst + count], ag_send.at[idx], ag_recv.at[idx], rel
        )

    c1, c2, c3 = chunk, 2 * chunk, 3 * chunk
    own_p = ag(0, 0, mine, mine, 1)
    x_h0 = ag(1, 0, c1, half, 2)
    y_h0 = ag(2, 0, c1 + half, half, 4)
    m1_p = ag(3, c1, c1 + mine, mine, 1)
    x_h1 = ag(4, half, c2, half, 2)
    y_h1 = ag(5, half, c2 + half, half, 4)
    m2_p = ag(6, c2, c2 + mine, mine, 1)
    d_x0 = ag(7, c1 + half, c3, quart, 2)
    d_y0 = ag(8, c1 + quart, c3 + quart, quart, 4)
    d_x1 = ag(9, c2 + half, c3 + half, quart, 2)
    d_y1 = ag(10, c2 + quart, c3 + half + quart, quart, 4)
    d_p = ag(11, c3, c3 + mine, mine, 1)
    metas = [remote(meta_v.at[0], meta_v.at[r], meta_send.at[r - 1], meta_recv.at[r - 1], r) for r in OTHERS]
    own_p.start()
    for copy in (*metas, x_h0, y_h0, x_h1, y_h1):
        copy.start()
    w_v[vocab_local:padded, :] = jnp.zeros((padded - vocab_local, width), jnp.bfloat16)
    last_top = vocab_local - (n_vt - 1) * VT
    z_o[n_vt // 2 - 1, last_top:VT, :] = jnp.full((VT - last_top, chunk), LOWEST, jnp.float32)

    base_f = (me * vocab_local).astype(jnp.float32)
    valid = jnp.minimum(vocab_local, vocab_real - me * vocab_local)

    def chunk_at(c):
        return pl.ds(pl.multiple_of(c * chunk, chunk), chunk)

    def row_at(row, c, lt):
        return row_v[row:row + 1, pl.ds(pl.multiple_of(c * chunk + lt * LANES, LANES), LANES)]

    def a_copy(c):
        return pltpu.make_async_copy(a_v.at[chunk_at(c)], a_out.at[chunk_at(c)], a_sem.at[c])

    def z_copy(c, j):
        return pltpu.make_async_copy(z_refs[j % 2].at[j // 2], z_hbm.at[c * n_vt + j], z_sem.at[j])

    groups = VT // GROUP

    def stats_pass(j):
        for lt in range(chunk // LANES):
            cols = slice(lt * LANES, (lt + 1) * LANES)
            for b in range(groups):
                z = z_refs[j % 2][j // 2, b * GROUP:(b + 1) * GROUP, cols].reshape(-1, SUBLANES, LANES)
                m = jnp.max(z, axis=0)
                at = (j * groups + b) // 2 * 8
                to = slice(b % 2 * chunk + lt * LANES, b % 2 * chunk + (lt + 1) * LANES)
                stat_v[0, at:at + 8, to] = m
                stat_v[1, at:at + 8, to] = jnp.sum(jnp.exp(z - m[None]), axis=0)

    def st_copy(c, r):
        at = c * 7 + r - 1
        return remote(st_v.at[0, c], st_v.at[r, c], st_send.at[at], st_recv.at[at], r)

    def send_stats(c):
        m = stat_v[0]
        m_col = jnp.max(m, axis=0, keepdims=True)
        m_row = jnp.maximum(m_col[:, :chunk], m_col[:, chunk:])
        s_col = jnp.sum(stat_v[1] * jnp.exp(m - jnp.concatenate([m_row, m_row], axis=1)), axis=0, keepdims=True)
        st_v[0, c, :, :chunk] = m_row
        st_v[0, c, :, chunk:] = s_col[:, :chunk] + s_col[:, chunk:]
        for r in OTHERS:
            st_copy(c, r).start()

    def logits(c, j, first, count):
        tokens = pl.ds(pl.multiple_of(c * chunk + first, mine), count)
        top = min(VT, vocab_local - j * VT)
        z_refs[j % 2][j // 2, :top, first:first + count] = lax.dot_general(
            w_v[j * VT:j * VT + top, :], a_v[tokens, :], (((1,), (1,)), ((), ())),
            preferred_element_type=jnp.float32,
        )

    def forward_chunk(c, carry):
        @pl.when(c == 0)
        def _():
            w_copy(0).wait()
            w_copy(1).wait()

        @pl.when(c == 1)
        def _():
            x_h0.wait_recv()
            y_h0.wait_recv()
            m1_p.start()
            d_x0.start()
            d_y0.start()

        @pl.when(c == 2)
        def _():
            x_h1.wait_recv()
            y_h1.wait_recv()
            m2_p.start()
            d_x1.start()
            d_y1.start()

        @pl.when(c == 3)
        def _():
            for copy in (d_x0, d_y0, d_x1, d_y1):
                copy.wait_recv()
            d_p.start()

        before = jnp.maximum(c - 1, 0)

        @pl.when(c > 0)
        def _():
            z_copy(before, 0).wait()
            z_copy(before, 1).wait()

        logits(c, 0, 0, mine)
        logits(c, 1, 0, mine)
        stats_pass(3)

        @pl.when(c > 0)
        def _():
            send_stats(before)

        @pl.when(c == 0)
        def _():
            for copy in metas:
                copy.wait_recv()
            for rel in RELS:
                for h in range(2):
                    u = unit_of(rel, h)
                    for row in range(2):
                        at = row * tok_dev + h * LANES
                        row_v[row:row + 1, u * LANES:(u + 1) * LANES] = meta_v[rel, :, at:at + LANES]
            local = row_v[:1, :] - base_f
            row_v[:1, :] = jnp.where(local < float(vocab_local), local, -1.0)
            own_p.wait_recv()

        for cc, copy in ((1, m1_p), (2, m2_p), (3, d_p)):
            @pl.when(c == cc)
            def _():
                copy.wait_recv()

        a_copy(c).start()
        logits(c, 0, mine, mine)
        logits(c, 1, mine, mine)

        @pl.when(c < 3)
        def _():
            z_copy(c, 0).start()
            z_copy(c, 1).start()

        for j in range(2, n_vt):
            @pl.when(c == 0)
            def _():
                w_copy(j).wait()

            @pl.when(c > 0)
            def _():
                z_copy(before, j).wait()

            logits(c, j, 0, chunk)
            stats_pass(j - 2)
            if j == n_vt - 1:
                stats_pass(j - 1)
                low = (vocab_local - PAD_COLS) // 8 * 8 - j * VT
                ids = j * VT + low + lax.broadcasted_iota(jnp.int32, (last_top - low, chunk), 0)
                z_o[j // 2, low:last_top, :] = jnp.where(ids < valid, z_o[j // 2, low:last_top, :], LOWEST)

            @pl.when(c < 3)
            def _():
                z_copy(c, j).start()

        return carry

    lax.fori_loop(0, 4, forward_chunk, 0)
    stats_pass(3)
    send_stats(3)

    for copy in (x_h0, y_h0, own_p, x_h1, y_h1, m1_p, m2_p, d_x0, d_y0, d_x1, d_y1, d_p):
        copy.wait_send()
    for c in range(4):
        a_copy(c).wait()

    w_row = row_v[1:2, :]
    row_v[3:4, :] = w_row / jnp.sum(w_row)
    for c in range(4):
        for r in OTHERS:
            st_copy(c, r).wait_recv()
    for rel in RELS:
        for h in range(2):
            parts = []
            for r in RELS:
                c, lt = divmod(unit_of(rel ^ r, h), 4)
                parts.append([st_v[r, c, :, at:at + LANES] for at in (lt * LANES, chunk + lt * LANES)])
            row_max = functools.reduce(jnp.maximum, [m for m, _ in parts])
            row_sum = sum(part * jnp.exp(m - row_max) for m, part in parts)
            u = unit_of(rel, h)
            row_v[2:3, u * LANES:(u + 1) * LANES] = row_max + jnp.log(row_sum)

    half_words = 2 * VT
    word_f = lax.broadcasted_iota(jnp.int32, (LANES, LANES), 0).astype(jnp.float32)

    def dz_pass(c, j, parity):
        out_at = parity * 2 + j
        for lt in range(chunk // LANES):
            cols = slice(lt * LANES, (lt + 1) * LANES)
            log_norm, scale = row_at(2, c, lt), row_at(3, c, lt)
            lab = row_at(0, c, lt) - jnp.float32(j * half_words) - word_f
            to_a = pl.ds(pl.multiple_of(out_at * chunk + lt * LANES, LANES), LANES)
            target = jnp.zeros((SUBLANES, LANES), jnp.float32)
            for b in range(0, half_words, LANES):
                z = z_refs[b // VT][j, b % VT:b % VT + LANES, cols]
                hit = lab == float(b)
                target += jnp.sum(jnp.where(hit, z, 0.0).reshape(-1, SUBLANES, LANES), axis=0)
                d = ((jnp.exp(z - log_norm) - jnp.where(hit, 1.0, 0.0)) * scale).astype(jnp.bfloat16)
                a_v[b:b + LANES, to_a] = d
                to_dz = pl.ds(pl.multiple_of(j * half_words + b, LANES), LANES)
                dz_refs[parity][cols, to_dz] = jnp.transpose(d)
            t_v[c, j, :, cols] = jnp.sum(target, axis=0, keepdims=True)

    def dz_copy(c, j, parity):
        out_at = parity * 2 + j
        src = a_v.at[:half_words, pl.ds(pl.multiple_of(out_at * chunk, chunk), chunk)]
        dst = dz_out.at[pl.ds(pl.multiple_of(j * half_words, half_words), half_words), chunk_at(c)]
        return pltpu.make_async_copy(src, dst, dz_sem.at[out_at])

    def z_reload(c, j):
        return [
            pltpu.make_async_copy(z_hbm.at[c * n_vt + 2 * j + i], z_refs[i].at[j], z_sem.at[2 * j + i])
            for i in range(2)
        ]

    def prt_copy(slot):
        return remote(out_v.at[slot, mine:chunk], prt_v.at[slot], prt_send.at[slot], prt_recv.at[slot], 1)

    def d_copy(route, j):
        return remote(
            dsend_v.at[j, route * half:(route + 1) * half], drecv_v.at[route, j],
            d_send.at[route * 2 + j], d_recv.at[route * 2 + j], 2 << route,
        )

    def e_copy(route):
        early = stat_v.at[route, :, :EARLY]
        return remote(first_v.at[route, 0, :, :EARLY], early, e_send.at[route], e_recv.at[route], 2 << route)

    outs = (px_out, py_out)

    def put_first(route, j):
        src = first_v.at[route, 1] if j else first_v.at[route, 0, :, EARLY:]
        dst = outs[route].at[:, NT - EARLY:2 * NT - EARLY] if j else outs[route].at[:, :NT - EARLY]
        return pltpu.make_async_copy(src, dst, put_sem.at[route * 2 + j])

    def put_hold(route, j):
        at = width - EARLY + j * NT
        return pltpu.make_async_copy(
            hold_v.at[route, j], outs[route].at[:, at:at + NT], put_sem.at[4 + route * 2 + j]
        )

    def put_own(j):
        return pltpu.make_async_copy(
            out_v.at[j, :mine], pown_out.at[:, j * NT:(j + 1) * NT], put_sem.at[8 + j]
        )

    def combine(s):
        slot = s % 2
        prt_copy(slot).wait_recv()
        for q in range(4):
            for j in range(2):
                @pl.when(s == 2 * q + j)
                def _():
                    if q == 0:
                        dsend_v[j] = out_v[j, :mine, :] + prt_v[j]
                        d_copy(0, j).start()
                        d_copy(1, j).start()
                    elif q == 3:
                        out_v[j, :mine, :] += prt_v[j]
                    else:
                        hold_at, first_at = ((0, half), (half, 0))[q - 1]
                        hold_to, first_to = ((0, 1), (1, 0))[q - 1]
                        hold_v[hold_to, j] = out_v[j, hold_at:hold_at + half, :] + prt_v[j, hold_at:hold_at + half, :]
                        first_v[first_to, j] = (
                            out_v[j, first_at:first_at + half, :] + prt_v[j, first_at:first_at + half, :]
                        )
                        if j == 0:
                            e_copy(first_to).start()
                        put_first(first_to, j).start()

        @pl.when(s < 6)
        def _():
            pl.semaphore_signal(credit, inc=1, device_id={"vp": peers[1]}, device_id_type=MESH)

    def backward_step(q, j, parity):
        s = 2 * q + j
        after = jnp.maximum(2 - q, 0)

        @pl.when((q >= 1) & (q < 3))
        def _():
            for copy in z_reload(after, j):
                copy.wait()

        @pl.when(q == 0)
        def _():
            for copy in z_reload(2, j):
                copy.wait()
            dz_copy(3, j, 0).start()

        @pl.when(q >= 1)
        def _():
            dz_copy(4 - q, j, 1 - parity).wait()
            prt_copy(j).wait_send()

        cols = pl.ds(pl.multiple_of(j * NT, NT), NT)
        out_v[j] = jnp.dot(dz_refs[parity][...], w_v[:, cols], preferred_element_type=jnp.float32)
        dz_pass(after, j, 1 - parity)

        @pl.when(q < 2)
        def _():
            for copy in z_reload(1 - q, j):
                copy.start()

        @pl.when(q < 3)
        def _():
            dz_copy(2 - q, j, 1 - parity).start()

        combine(s - 1)

        @pl.when(s >= 2)
        def _():
            pl.semaphore_wait(credit, 1)

        prt_copy(j).start()

    def first_product(j):
        words = slice(j * half_words, (j + 1) * half_words)
        return jnp.dot(dz_e[:, words], w_v[words, :NT], preferred_element_type=jnp.float32)

    dz_pass(3, 0, 0)
    for copy in z_reload(2, 0):
        copy.start()
    out_v[0] = first_product(0)
    dz_pass(3, 1, 0)
    for copy in z_reload(2, 0):
        copy.wait()
    for copy in z_reload(2, 1):
        copy.start()
    dz_copy(3, 0, 0).start()
    out_v[0] += first_product(1)
    dz_pass(2, 0, 1)
    for copy in z_reload(1, 0):
        copy.start()
    dz_copy(2, 0, 1).start()
    prt_copy(0).start()

    def backward_pair(qq, carry):
        for parity in range(2):
            def step(j, inner):
                backward_step(2 * qq + parity, j, parity)
                return inner
            lax.fori_loop(jnp.maximum(1 - qq, 0) if parity == 0 else 0, 2, step, 0)
        return carry

    lax.fori_loop(0, 2, backward_pair, 0)
    combine(jnp.int32(7))

    loss = jnp.zeros((1, LANES), jnp.float32)
    for u in range(tokens // LANES):
        cols = slice(u * LANES, (u + 1) * LANES)
        c, lt = divmod(u, 4)
        at = slice(lt * LANES, (lt + 1) * LANES)
        targets = t_v[c, 0, :, at] + t_v[c, 1, :, at]
        own_norm = row_v[2:3, cols] if u < tok_dev // LANES else 0.0
        loss += row_v[3:4, cols] * (own_norm - targets)
    loss_v[...] = loss
    loss_copy.start()

    for j in range(2):
        for route in range(2):
            d_copy(route, j).wait_recv()
            hold_v[1 - route, j] += drecv_v[route, j]
            put_hold(1 - route, j).start()
    put_own(1).start()
    for route in range(2):
        e_copy(route).wait_recv()
        out_v[0, route * half:(route + 1) * half, :EARLY] += stat_v[route, :, :EARLY]
    put_own(0).start()

    loss_copy.wait()
    for copy in metas:
        copy.wait_send()
    for c in range(4):
        for r in OTHERS:
            st_copy(c, r).wait_send()
    for j in range(2):
        prt_copy(j).wait_send()
        dz_copy(0, j, 1).wait()
        put_own(j).wait()
        e_copy(j).wait_send()
        for route in range(2):
            d_copy(route, j).wait_send()
            put_first(route, j).wait()
            put_hold(route, j).wait()


def head(hidden, labels, loss_weight, norm_gain, w_t):
    tok_dev, width = hidden.shape
    tokens = 8 * tok_dev
    vocab_local = w_t.shape[0]
    padded = -(-vocab_local // VT) * VT
    chunk = 2 * tok_dev
    n_vt = padded // VT
    half = tok_dev // 2
    f32, bf16 = jnp.float32, jnp.bfloat16
    hbm = pl.BlockSpec(memory_space=pltpu.MemorySpace.HBM)
    dma = pltpu.SemaphoreType.DMA
    return pl.pallas_call(
        head_kernel,
        out_shape=[
            jax.ShapeDtypeStruct((tokens, width), bf16),
            jax.ShapeDtypeStruct((padded, tokens), bf16),
            jax.ShapeDtypeStruct((half, 2 * width - EARLY), f32),
            jax.ShapeDtypeStruct((half, 2 * width - EARLY), f32),
            jax.ShapeDtypeStruct((tok_dev, width), f32),
            jax.ShapeDtypeStruct((3 * n_vt, VT, chunk), f32),
            jax.ShapeDtypeStruct((1, LANES), f32),
        ],
        in_specs=[hbm] * 5,
        out_specs=[hbm] * 7,
        scratch_shapes=[
            pltpu.VMEM((1, tok_dev), labels.dtype),
            *[pltpu.VMEM((1, count), f32) for count in (tok_dev, width, LANES)],
            pltpu.VMEM((padded, width), bf16),
            pltpu.VMEM((tokens, width), bf16),
            *[pltpu.VMEM((n_vt // 2, VT, chunk), f32) for _ in "eo"],
            *[pltpu.VMEM((chunk, padded), bf16) for _ in "eo"],
            pltpu.VMEM((8, 1, chunk), f32),
            pltpu.VMEM((8, tokens), f32),
            pltpu.VMEM((2, half, NT), f32),
            pltpu.VMEM((4, 2, 1, chunk), f32),
            pltpu.VMEM((8, 4, 1, 2 * chunk), f32),
            pltpu.VMEM((2, chunk, NT), f32),
            pltpu.VMEM((2, tok_dev, NT), f32),
            pltpu.VMEM((2, 2, half, NT), f32),
            pltpu.VMEM((2, tok_dev, NT), f32),
            *[pltpu.VMEM((2, 2, half, NT), f32) for _ in "hf"],
            *[dma((count,)) for count in (12, 7, 28, 2, 4, 2) for _ in "sr"],
            dma((5,)), dma((n_vt,)), dma((n_vt,)), dma((4,)), dma((4,)), dma((10,)),
            pltpu.SemaphoreType.REGULAR,
        ],
        compiler_params=pltpu.CompilerParams(
            collective_id=0, has_side_effects=True, vmem_limit_bytes=VMEM_BYTES,
        ),
        cost_estimate=pl.CostEstimate(
            flops=4 * tokens * width * padded, bytes_accessed=120_000_000, transcendentals=2 * tokens * padded
        ),
        name="head",
    )(hidden, labels[None], loss_weight[None], norm_gain[None], w_t)


def tail_kernel(
    hidden_hbm, gain_ref, own_hbm, x_hbm, y_hbm, loss_ref, dh_hbm, dgain_ref, total_ref,
    h_v, g_v, x_v, y_v, dh_v, buf, in_sem, out_sem, send, recv
):
    me = lax.axis_index("vp")
    peers = xor_peers(me)
    barrier = pltpu.get_barrier_semaphore()
    for r in OTHERS:
        pl.semaphore_signal(barrier, inc=1, device_id={"vp": peers[r]}, device_id_type=MESH)
    rows, width = hidden_hbm.shape
    half = rows // 2
    rest_at = x_hbm.shape[1] - width
    early = width - rest_at
    step = 64

    def loads(k):
        at = slice(k * step, (k + 1) * step)
        here = slice(k * step % half, k * step % half + step)
        x_cols, y_cols = slice(0, rest_at), slice(rest_at, rest_at + width)
        if k * step >= half:
            x_cols, y_cols = y_cols, x_cols
        return [
            pltpu.make_async_copy(hidden_hbm.at[at], h_v.at[at], in_sem.at[k, 0]),
            pltpu.make_async_copy(own_hbm.at[at], g_v.at[at], in_sem.at[k, 1]),
            pltpu.make_async_copy(x_hbm.at[here, x_cols], x_v.at[here, x_cols], in_sem.at[k, 2]),
            pltpu.make_async_copy(y_hbm.at[here, y_cols], y_v.at[here, y_cols], in_sem.at[k, 3]),
        ]

    for k in range(rows // step):
        for copy in loads(k):
            copy.start()
    acc = jnp.zeros((SUBLANES, width), jnp.float32)
    for b in range(0, rows, 32):
        if b % step == 0:
            for copy in loads(b // step):
                copy.wait()
        at = slice(b, b + 32)
        here = slice(b % half, b % half + 32)
        part, rest = (x_v, y_v) if b < half else (y_v, x_v)
        x = h_v[at, :].astype(jnp.float32)
        inv_rms = lax.rsqrt(jnp.mean(x * x, axis=-1, keepdims=True) + NORM_EPS)
        own = g_v[at, :] + rest[here, rest_at:rest_at + width]
        g = jnp.concatenate([own[:, :early], own[:, early:] + part[here, :rest_at]], axis=1)
        g_v[at, :] = g
        gn = g * (x * inv_rms)
        for i in range(0, 32, 8):
            acc += gn[i:i + 8, :]
    buf[0, :, :width] = jnp.sum(acc, axis=0, keepdims=True)
    buf[0, :, width:width + LANES] = loss_ref[...]
    pl.semaphore_wait(barrier, 7)
    copies = [
        pltpu.make_async_remote_copy(
            src_ref=buf.at[0], dst_ref=buf.at[r], send_sem=send.at[r - 1], recv_sem=recv.at[r - 1],
            device_id={"vp": peers[r]}, device_id_type=MESH,
        )
        for r in OTHERS
    ]
    for copy in copies:
        copy.start()
    for b in range(0, rows, 32):
        at = slice(b, b + 32)
        x = h_v[at, :].astype(jnp.float32)
        inv_rms = lax.rsqrt(jnp.mean(x * x, axis=-1, keepdims=True) + NORM_EPS)
        n = x * inv_rms
        u = g_v[at, :] * gain_ref[...]
        dh_v[at, :] = (inv_rms * (u - n * jnp.mean(u * n, axis=-1, keepdims=True))).astype(jnp.bfloat16)
    dh_copy = pltpu.make_async_copy(dh_v, dh_hbm, out_sem)
    dh_copy.start()
    for copy in copies:
        copy.wait()
    pairs = [buf[2 * r] + buf[2 * r + 1] for r in range(4)]
    total = (pairs[0] + pairs[1]) + (pairs[2] + pairs[3])
    dgain_ref[...] = total[:, :width]
    total_ref[...] = jnp.broadcast_to(jnp.sum(total[:, width:], axis=1, keepdims=True), total_ref.shape)
    dh_copy.wait()


def tail(hidden, norm_gain, own, from_x, from_y, loss):
    tok_dev, width = hidden.shape
    whole = pl.BlockSpec(memory_space=pltpu.VMEM)
    hbm = pl.BlockSpec(memory_space=pltpu.MemorySpace.HBM)
    return pl.pallas_call(
        tail_kernel,
        out_shape=[
            jax.ShapeDtypeStruct((tok_dev, width), jnp.bfloat16),
            jax.ShapeDtypeStruct((1, width), jnp.float32),
            jax.ShapeDtypeStruct((1, LANES), jnp.float32),
        ],
        in_specs=[hbm, whole, hbm, hbm, hbm, whole],
        out_specs=[hbm, whole, whole],
        scratch_shapes=[
            pltpu.VMEM((tok_dev, width), jnp.bfloat16),
            pltpu.VMEM((tok_dev, width), jnp.float32),
            pltpu.VMEM(from_x.shape, jnp.float32),
            pltpu.VMEM(from_y.shape, jnp.float32),
            pltpu.VMEM((tok_dev, width), jnp.bfloat16),
            pltpu.VMEM((8, 1, width + LANES), jnp.float32),
            pltpu.SemaphoreType.DMA((4, 4)),
            pltpu.SemaphoreType.DMA,
            *[pltpu.SemaphoreType.DMA((7,)) for _ in "sr"],
        ],
        compiler_params=pltpu.CompilerParams(collective_id=1, has_side_effects=True),
        cost_estimate=pl.CostEstimate(flops=10 * tok_dev * width, bytes_accessed=8_000_000, transcendentals=0),
        name="tail",
    )(hidden, norm_gain[None], own, from_x, from_y, loss)


def finish_kernel(dh_ref, dgain_ref, loss_ref, dh_out, dgain_out, loss_out):
    dh_out[...] = dh_ref[...]
    dgain_out[...] = dgain_ref[...]
    loss_out[...] = loss_ref[:, :1]


def finish(dh, dgain, loss):
    whole = pl.BlockSpec(memory_space=pltpu.VMEM)
    return pl.pallas_call(
        finish_kernel,
        out_shape=[
            jax.ShapeDtypeStruct(dh.shape, dh.dtype),
            jax.ShapeDtypeStruct(dgain.shape, dgain.dtype),
            jax.ShapeDtypeStruct((1, 1), loss.dtype),
        ],
        in_specs=[whole] * 3,
        out_specs=[whole] * 3,
        name="finish",
    )(dh, dgain, loss)


def weight_grad_kernel(dz_hbm, a_hbm, out_hbm, dz_v, a_v, out_v, dz_sem, a_sem, out_sem):
    vocab_local = out_hbm.shape[0]
    n_vt = dz_hbm.shape[0] // VT

    def dz_copy(v):
        return pltpu.make_async_copy(
            dz_hbm.at[pl.ds(pl.multiple_of(v * VT, VT), VT)], dz_v.at[v % 2], dz_sem.at[v % 2]
        )

    def a_copy(d):
        return pltpu.make_async_copy(a_hbm.at[:, d * NT:(d + 1) * NT], a_v.at[:, d * NT:(d + 1) * NT], a_sem.at[d])

    def out_copy(v, d, count):
        return pltpu.make_async_copy(
            out_v.at[d, :count],
            out_hbm.at[pl.ds(pl.multiple_of(v * VT, VT), count), pl.ds(pl.multiple_of(d * NT, NT), NT)],
            out_sem.at[d],
        )

    last_count = vocab_local - (n_vt - 1) * VT
    dz_copy(0).start()
    a_copy(0).start()
    a_copy(1).start()
    dz_copy(1).start()

    def step(i, carry):
        v, d = i // 2, i % 2

        @pl.when(d == 0)
        def _():
            dz_copy(v).wait()

        for dd in range(2):
            @pl.when(i == dd)
            def _():
                a_copy(dd).wait()

        @pl.when(i >= 2)
        def _():
            out_copy(v - 1, d, VT).wait()

        cols = pl.ds(pl.multiple_of(d * NT, NT), NT)
        out_v[d] = jnp.dot(dz_v[v % 2], a_v[:, cols], preferred_element_type=jnp.float32)

        @pl.when(v < n_vt - 1)
        def _():
            out_copy(v, d, VT).start()

        @pl.when(v == n_vt - 1)
        def _():
            out_copy(v, d, last_count).start()

        @pl.when((d == 1) & (v < n_vt - 2))
        def _():
            dz_copy(v + 2).start()

        return carry

    lax.fori_loop(0, 2 * n_vt, step, 0)
    for d in range(2):
        out_copy(n_vt - 1, d, last_count).wait()


def weight_grad(dz_t, a_all, vocab_local):
    tokens, width = a_all.shape
    padded = dz_t.shape[0]
    hbm = pl.BlockSpec(memory_space=pltpu.MemorySpace.HBM)
    return pl.pallas_call(
        weight_grad_kernel,
        out_shape=jax.ShapeDtypeStruct((vocab_local, width), jnp.float32),
        in_specs=[hbm, hbm],
        out_specs=hbm,
        scratch_shapes=[
            pltpu.VMEM((2, VT, tokens), jnp.bfloat16),
            pltpu.VMEM((tokens, width), jnp.bfloat16),
            pltpu.VMEM((2, VT, NT), jnp.float32),
            *[pltpu.SemaphoreType.DMA((2,)) for _ in "dao"],
        ],
        compiler_params=pltpu.CompilerParams(vmem_limit_bytes=VMEM_BYTES),
        cost_estimate=pl.CostEstimate(
            flops=2 * tokens * width * padded, bytes_accessed=60_000_000, transcendentals=0
        ),
        name="weight_grad",
    )(dz_t, a_all)


def solution(mesh):
    group_size = mesh.shape["vp"]

    def local_step(hidden, labels, loss_weight, norm_gain, w_local):
        vocab_local = w_local.shape[1]
        a_all, dz_t, px, py, pown, _, loss = head(hidden, labels, loss_weight, norm_gain, w_local.T)
        from_x = lax.ppermute(px, "vp", [(i, i ^ 2) for i in range(group_size)])
        from_y = lax.ppermute(py, "vp", [(i, i ^ 4) for i in range(group_size)])
        d_unembed = weight_grad(dz_t, a_all, vocab_local).T
        small = tail(hidden, norm_gain, pown, from_x, from_y, loss)
        d_input, d_gain, mean_loss = finish(*small)
        return mean_loss[0], d_input, d_unembed, d_gain[0]

    return jax.shard_map(
        local_step,
        mesh=mesh,
        in_specs=(P(("dp", "vp"), None), P(("dp", "vp")), P(("dp", "vp")), P(None), P(None, "vp")),
        out_specs=(P("dp"), P(("dp", "vp"), None), P("dp", "vp"), P("dp")),
        check_vma=False,
    )
```

```python
import functools

import jax
import jax.numpy as jnp
from jax import lax
from jax.experimental import pallas as pl
from jax.experimental.pallas import tpu as pltpu
from jax.sharding import PartitionSpec as P

NORM_EPS = 1e-5
PAD_COLS = 128
LANES = 128
VT = 1024
NT = 1024
EARLY = 512
GROUP = 128
MESH = pl.DeviceIdType.MESH
VMEM_BYTES = 67_043_328
LOWEST = -3.0e38
SMALL_BYTES = 24_000_000
SUBLANES = 8
RELS = range(8)
OTHERS = RELS[1:]


def xor_peers(me):
    step_core = 1 - 2 * (me % 2)
    step_x = 2 - 4 * ((me // 2) % 2)
    step_y = 4 - 8 * (me // 4)
    return [me + (r % 2) * step_core + ((r // 2) % 2) * step_x + (r // 4) * step_y for r in RELS]


def unit_of(rel, half):
    if rel in (0, 1):
        return 2 * rel + half
    if rel in (6, 7):
        return 12 + 2 * (rel - 6) + half
    return {2: 4, 4: 5, 3: 6, 5: 7}[rel] + 4 * half


def head_kernel(
    hidden_hbm, label_hbm, weight_hbm, gain_hbm, w_hbm,
    a_out, dz_out, px_out, py_out, pown_out, z_hbm, loss_out,
    label_v, weight_v, gain_v, loss_v, w_v, a_v, z_e, z_o, dz_e, dz_o, meta_v, row_v, stat_v, t_v, st_v,
    out_v, prt_v, drecv_v, dsend_v, hold_v, first_v,
    ag_send, ag_recv, meta_send, meta_recv, st_send, st_recv, prt_send, prt_recv, d_send, d_recv, e_send, e_recv,
    in_sem, w_sem, z_sem, a_sem, dz_sem, put_sem, credit,
):
    me = lax.axis_index("vp")
    peers = xor_peers(me)
    vocab_local, width = w_hbm.shape
    vocab_real = 8 * vocab_local - PAD_COLS
    padded = w_v.shape[0]
    n_vt = padded // VT
    tok_dev = hidden_hbm.shape[0]
    chunk = 2 * tok_dev
    half = tok_dev // 2
    quart = tok_dev // 4
    tokens = 4 * chunk
    mine = tok_dev
    z_refs = (z_e, z_o)
    dz_refs = (dz_e, dz_o)

    def remote(src, dst, send, recv, rel):
        return pltpu.make_async_remote_copy(
            src_ref=src, dst_ref=dst, send_sem=send, recv_sem=recv,
            device_id={"vp": peers[rel]}, device_id_type=MESH,
        )

    hidden_v = dz_e.at[:tok_dev, :width]
    small = ((hidden_hbm, hidden_v), (label_hbm, label_v), (weight_hbm, weight_v), (gain_hbm, gain_v), (loss_v, loss_out))
    *ins, loss_copy = [pltpu.make_async_copy(src, dst, in_sem.at[i]) for i, (src, dst) in enumerate(small)]
    for copy in ins:
        copy.start()
    barrier = pltpu.get_barrier_semaphore()
    for r in OTHERS:
        pl.semaphore_signal(barrier, inc=1, device_id={"vp": peers[r]}, device_id_type=MESH)

    def w_copy(j):
        hi = min((j + 1) * VT, vocab_local)
        return pltpu.make_async_copy(w_hbm.at[j * VT:hi], w_v.at[j * VT:hi], w_sem.at[j])

    for j in range(n_vt):
        w_copy(j).start()

    for copy in ins:
        copy.wait()
    meta_v[0, :, :tok_dev] = label_v[...].astype(jnp.float32)
    meta_v[0, :, tok_dev:chunk] = weight_v[...]
    for b in range(0, tok_dev, 32):
        x = dz_e[b:b + 32, :width].astype(jnp.float32)
        inv_rms = lax.rsqrt(jnp.mean(x * x, axis=-1, keepdims=True) + NORM_EPS)
        a_v[b:b + 32, :] = (x * inv_rms * gain_v[...]).astype(jnp.bfloat16)
    pl.semaphore_wait(barrier, 7)

    def ag(idx, src, dst, count, rel):
        return remote(
            a_v.at[src:src + count], a_v.at[dst:dst + count], ag_send.at[idx], ag_recv.at[idx], rel
        )

    c1, c2, c3 = chunk, 2 * chunk, 3 * chunk
    own_p = ag(0, 0, mine, mine, 1)
    x_h0 = ag(1, 0, c1, half, 2)
    y_h0 = ag(2, 0, c1 + half, half, 4)
    m1_p = ag(3, c1, c1 + mine, mine, 1)
    x_h1 = ag(4, half, c2, half, 2)
    y_h1 = ag(5, half, c2 + half, half, 4)
    m2_p = ag(6, c2, c2 + mine, mine, 1)
    d_x0 = ag(7, c1 + half, c3, quart, 2)
    d_y0 = ag(8, c1 + quart, c3 + quart, quart, 4)
    d_x1 = ag(9, c2 + half, c3 + half, quart, 2)
    d_y1 = ag(10, c2 + quart, c3 + half + quart, quart, 4)
    d_p = ag(11, c3, c3 + mine, mine, 1)
    metas = [remote(meta_v.at[0], meta_v.at[r], meta_send.at[r - 1], meta_recv.at[r - 1], r) for r in OTHERS]
    own_p.start()
    for copy in (*metas, x_h0, y_h0, x_h1, y_h1):
        copy.start()
    w_v[vocab_local:padded, :] = jnp.zeros((padded - vocab_local, width), jnp.bfloat16)
    last_top = vocab_local - (n_vt - 1) * VT
    z_o[n_vt // 2 - 1, last_top:VT, :] = jnp.full((VT - last_top, chunk), LOWEST, jnp.float32)

    base_f = (me * vocab_local).astype(jnp.float32)
    valid = jnp.minimum(vocab_local, vocab_real - me * vocab_local)

    def chunk_at(c):
        return pl.ds(pl.multiple_of(c * chunk, chunk), chunk)

    def row_at(row, c, lt):
        return row_v[row:row + 1, pl.ds(pl.multiple_of(c * chunk + lt * LANES, LANES), LANES)]

    def a_copy(c):
        return pltpu.make_async_copy(a_v.at[chunk_at(c)], a_out.at[chunk_at(c)], a_sem.at[c])

    def z_copy(c, j):
        return pltpu.make_async_copy(z_refs[j % 2].at[j // 2], z_hbm.at[c * n_vt + j], z_sem.at[j])

    groups = VT // GROUP

    def stats_pass(j):
        for lt in range(chunk // LANES):
            cols = slice(lt * LANES, (lt + 1) * LANES)
            for b in range(groups):
                z = z_refs[j % 2][j // 2, b * GROUP:(b + 1) * GROUP, cols].reshape(-1, SUBLANES, LANES)
                m = jnp.max(z, axis=0)
                at = (j * groups + b) // 2 * 8
                to = slice(b % 2 * chunk + lt * LANES, b % 2 * chunk + (lt + 1) * LANES)
                stat_v[0, at:at + 8, to] = m
                stat_v[1, at:at + 8, to] = jnp.sum(jnp.exp(z - m[None]), axis=0)

    def st_copy(c, r):
        at = c * 7 + r - 1
        return remote(st_v.at[0, c], st_v.at[r, c], st_send.at[at], st_recv.at[at], r)

    def send_stats(c):
        m = stat_v[0]
        m_col = jnp.max(m, axis=0, keepdims=True)
        m_row = jnp.maximum(m_col[:, :chunk], m_col[:, chunk:])
        s_col = jnp.sum(stat_v[1] * jnp.exp(m - jnp.concatenate([m_row, m_row], axis=1)), axis=0, keepdims=True)
        st_v[0, c, :, :chunk] = m_row
        st_v[0, c, :, chunk:] = s_col[:, :chunk] + s_col[:, chunk:]
        for r in OTHERS:
            st_copy(c, r).start()

    def logits(c, j, first, count):
        tokens = pl.ds(pl.multiple_of(c * chunk + first, mine), count)
        top = min(VT, vocab_local - j * VT)
        z_refs[j % 2][j // 2, :top, first:first + count] = lax.dot_general(
            w_v[j * VT:j * VT + top, :], a_v[tokens, :], (((1,), (1,)), ((), ())),
            preferred_element_type=jnp.float32,
        )

    def forward_chunk(c, carry):
        @pl.when(c == 0)
        def _():
            w_copy(0).wait()
            w_copy(1).wait()

        @pl.when(c == 1)
        def _():
            x_h0.wait_recv()
            y_h0.wait_recv()
            m1_p.start()
            d_x0.start()
            d_y0.start()

        @pl.when(c == 2)
        def _():
            x_h1.wait_recv()
            y_h1.wait_recv()
            m2_p.start()
            d_x1.start()
            d_y1.start()

        @pl.when(c == 3)
        def _():
            for copy in (d_x0, d_y0, d_x1, d_y1):
                copy.wait_recv()
            d_p.start()

        before = jnp.maximum(c - 1, 0)

        @pl.when(c > 0)
        def _():
            z_copy(before, 0).wait()
            z_copy(before, 1).wait()

        logits(c, 0, 0, mine)
        logits(c, 1, 0, mine)
        stats_pass(3)

        @pl.when(c > 0)
        def _():
            send_stats(before)

        @pl.when(c == 0)
        def _():
            for copy in metas:
                copy.wait_recv()
            for rel in RELS:
                for h in range(2):
                    u = unit_of(rel, h)
                    for row in range(2):
                        at = row * tok_dev + h * LANES
                        row_v[row:row + 1, u * LANES:(u + 1) * LANES] = meta_v[rel, :, at:at + LANES]
            local = row_v[:1, :] - base_f
            row_v[:1, :] = jnp.where(local < float(vocab_local), local, -1.0)
            own_p.wait_recv()

        for cc, copy in ((1, m1_p), (2, m2_p), (3, d_p)):
            @pl.when(c == cc)
            def _():
                copy.wait_recv()

        a_copy(c).start()
        logits(c, 0, mine, mine)
        logits(c, 1, mine, mine)

        @pl.when(c < 3)
        def _():
            z_copy(c, 0).start()
            z_copy(c, 1).start()

        for j in range(2, n_vt):
            @pl.when(c == 0)
            def _():
                w_copy(j).wait()

            @pl.when(c > 0)
            def _():
                z_copy(before, j).wait()

            logits(c, j, 0, chunk)
            stats_pass(j - 2)
            if j == n_vt - 1:
                stats_pass(j - 1)
                low = (vocab_local - PAD_COLS) // 8 * 8 - j * VT
                ids = j * VT + low + lax.broadcasted_iota(jnp.int32, (last_top - low, chunk), 0)
                z_o[j // 2, low:last_top, :] = jnp.where(ids < valid, z_o[j // 2, low:last_top, :], LOWEST)

            @pl.when(c < 3)
            def _():
                z_copy(c, j).start()

        return carry

    lax.fori_loop(0, 4, forward_chunk, 0)
    stats_pass(3)
    send_stats(3)

    for copy in (x_h0, y_h0, own_p, x_h1, y_h1, m1_p, m2_p, d_x0, d_y0, d_x1, d_y1, d_p):
        copy.wait_send()
    for c in range(4):
        a_copy(c).wait()

    w_row = row_v[1:2, :]
    row_v[3:4, :] = w_row / jnp.sum(w_row)
    for c in range(4):
        for r in OTHERS:
            st_copy(c, r).wait_recv()
    for rel in RELS:
        for h in range(2):
            parts = []
            for r in RELS:
                c, lt = divmod(unit_of(rel ^ r, h), 4)
                parts.append([st_v[r, c, :, at:at + LANES] for at in (lt * LANES, chunk + lt * LANES)])
            row_max = functools.reduce(jnp.maximum, [m for m, _ in parts])
            row_sum = sum(part * jnp.exp(m - row_max) for m, part in parts)
            u = unit_of(rel, h)
            row_v[2:3, u * LANES:(u + 1) * LANES] = row_max + jnp.log(row_sum)

    half_words = 2 * VT
    word_f = lax.broadcasted_iota(jnp.int32, (LANES, LANES), 0).astype(jnp.float32)

    def dz_pass(c, j, parity):
        out_at = parity * 2 + j
        for lt in range(chunk // LANES):
            cols = slice(lt * LANES, (lt + 1) * LANES)
            log_norm, scale = row_at(2, c, lt), row_at(3, c, lt)
            lab = row_at(0, c, lt) - jnp.float32(j * half_words) - word_f
            to_a = pl.ds(pl.multiple_of(out_at * chunk + lt * LANES, LANES), LANES)
            target = jnp.zeros((SUBLANES, LANES), jnp.float32)
            for b in range(0, half_words, LANES):
                z = z_refs[b // VT][j, b % VT:b % VT + LANES, cols]
                hit = lab == float(b)
                target += jnp.sum(jnp.where(hit, z, 0.0).reshape(-1, SUBLANES, LANES), axis=0)
                d = ((jnp.exp(z - log_norm) - jnp.where(hit, 1.0, 0.0)) * scale).astype(jnp.bfloat16)
                a_v[b:b + LANES, to_a] = d
                to_dz = pl.ds(pl.multiple_of(j * half_words + b, LANES), LANES)
                dz_refs[parity][cols, to_dz] = jnp.transpose(d)
            t_v[c, j, :, cols] = jnp.sum(target, axis=0, keepdims=True)

    def dz_copy(c, j, parity):
        out_at = parity * 2 + j
        src = a_v.at[:half_words, pl.ds(pl.multiple_of(out_at * chunk, chunk), chunk)]
        dst = dz_out.at[pl.ds(pl.multiple_of(j * half_words, half_words), half_words), chunk_at(c)]
        return pltpu.make_async_copy(src, dst, dz_sem.at[out_at])

    def z_reload(c, j):
        return [
            pltpu.make_async_copy(z_hbm.at[c * n_vt + 2 * j + i], z_refs[i].at[j], z_sem.at[2 * j + i])
            for i in range(2)
        ]

    def prt_copy(slot):
        return remote(out_v.at[slot, mine:chunk], prt_v.at[slot], prt_send.at[slot], prt_recv.at[slot], 1)

    def d_copy(route, j):
        return remote(
            dsend_v.at[j, route * half:(route + 1) * half], drecv_v.at[route, j],
            d_send.at[route * 2 + j], d_recv.at[route * 2 + j], 2 << route,
        )

    def e_copy(route):
        early = stat_v.at[route, :, :EARLY]
        return remote(first_v.at[route, 0, :, :EARLY], early, e_send.at[route], e_recv.at[route], 2 << route)

    outs = (px_out, py_out)

    def put_first(route, j):
        src = first_v.at[route, 1] if j else first_v.at[route, 0, :, EARLY:]
        dst = outs[route].at[:, NT - EARLY:2 * NT - EARLY] if j else outs[route].at[:, :NT - EARLY]
        return pltpu.make_async_copy(src, dst, put_sem.at[route * 2 + j])

    def put_hold(route, j):
        at = width - EARLY + j * NT
        return pltpu.make_async_copy(
            hold_v.at[route, j], outs[route].at[:, at:at + NT], put_sem.at[4 + route * 2 + j]
        )

    def put_own(j):
        return pltpu.make_async_copy(
            out_v.at[j, :mine], pown_out.at[:, j * NT:(j + 1) * NT], put_sem.at[8 + j]
        )

    def combine(s):
        slot = s % 2
        prt_copy(slot).wait_recv()
        for q in range(4):
            for j in range(2):
                @pl.when(s == 2 * q + j)
                def _():
                    if q == 0:
                        dsend_v[j] = out_v[j, :mine, :] + prt_v[j]
                        d_copy(0, j).start()
                        d_copy(1, j).start()
                    elif q == 3:
                        out_v[j, :mine, :] += prt_v[j]
                    else:
                        hold_at, first_at = ((0, half), (half, 0))[q - 1]
                        hold_to, first_to = ((0, 1), (1, 0))[q - 1]
                        hold_v[hold_to, j] = out_v[j, hold_at:hold_at + half, :] + prt_v[j, hold_at:hold_at + half, :]
                        first_v[first_to, j] = (
                            out_v[j, first_at:first_at + half, :] + prt_v[j, first_at:first_at + half, :]
                        )
                        if j == 0:
                            e_copy(first_to).start()
                        put_first(first_to, j).start()

        @pl.when(s < 6)
        def _():
            pl.semaphore_signal(credit, inc=1, device_id={"vp": peers[1]}, device_id_type=MESH)

    def backward_step(q, j, parity):
        s = 2 * q + j
        after = jnp.maximum(2 - q, 0)

        @pl.when((q >= 1) & (q < 3))
        def _():
            for copy in z_reload(after, j):
                copy.wait()

        @pl.when(q == 0)
        def _():
            for copy in z_reload(2, j):
                copy.wait()
            dz_copy(3, j, 0).start()

        @pl.when(q >= 1)
        def _():
            dz_copy(4 - q, j, 1 - parity).wait()
            prt_copy(j).wait_send()

        cols = pl.ds(pl.multiple_of(j * NT, NT), NT)
        out_v[j] = jnp.dot(dz_refs[parity][...], w_v[:, cols], preferred_element_type=jnp.float32)
        dz_pass(after, j, 1 - parity)

        @pl.when(q < 2)
        def _():
            for copy in z_reload(1 - q, j):
                copy.start()

        @pl.when(q < 3)
        def _():
            dz_copy(2 - q, j, 1 - parity).start()

        combine(s - 1)

        @pl.when(s >= 2)
        def _():
            pl.semaphore_wait(credit, 1)

        prt_copy(j).start()

    def first_product(j):
        words = slice(j * half_words, (j + 1) * half_words)
        return jnp.dot(dz_e[:, words], w_v[words, :NT], preferred_element_type=jnp.float32)

    dz_pass(3, 0, 0)
    for copy in z_reload(2, 0):
        copy.start()
    out_v[0] = first_product(0)
    dz_pass(3, 1, 0)
    for copy in z_reload(2, 0):
        copy.wait()
    for copy in z_reload(2, 1):
        copy.start()
    dz_copy(3, 0, 0).start()
    out_v[0] += first_product(1)
    dz_pass(2, 0, 1)
    for copy in z_reload(1, 0):
        copy.start()
    dz_copy(2, 0, 1).start()
    prt_copy(0).start()

    def backward_pair(qq, carry):
        for parity in range(2):
            def step(j, inner):
                backward_step(2 * qq + parity, j, parity)
                return inner
            lax.fori_loop(jnp.maximum(1 - qq, 0) if parity == 0 else 0, 2, step, 0)
        return carry

    lax.fori_loop(0, 2, backward_pair, 0)
    combine(jnp.int32(7))

    loss = jnp.zeros((1, LANES), jnp.float32)
    for u in range(tokens // LANES):
        cols = slice(u * LANES, (u + 1) * LANES)
        c, lt = divmod(u, 4)
        at = slice(lt * LANES, (lt + 1) * LANES)
        targets = t_v[c, 0, :, at] + t_v[c, 1, :, at]
        own_norm = row_v[2:3, cols] if u < tok_dev // LANES else 0.0
        loss += row_v[3:4, cols] * (own_norm - targets)
    loss_v[...] = loss
    loss_copy.start()

    for j in range(2):
        for route in range(2):
            d_copy(route, j).wait_recv()
            hold_v[1 - route, j] += drecv_v[route, j]
            put_hold(1 - route, j).start()
    put_own(1).start()
    for route in range(2):
        e_copy(route).wait_recv()
        out_v[0, route * half:(route + 1) * half, :EARLY] += stat_v[route, :, :EARLY]
    put_own(0).start()

    loss_copy.wait()
    for copy in metas:
        copy.wait_send()
    for c in range(4):
        for r in OTHERS:
            st_copy(c, r).wait_send()
    for j in range(2):
        prt_copy(j).wait_send()
        dz_copy(0, j, 1).wait()
        put_own(j).wait()
        e_copy(j).wait_send()
        for route in range(2):
            d_copy(route, j).wait_send()
            put_first(route, j).wait()
            put_hold(route, j).wait()


def head(hidden, labels, loss_weight, norm_gain, w_t):
    tok_dev, width = hidden.shape
    tokens = 8 * tok_dev
    vocab_local = w_t.shape[0]
    padded = -(-vocab_local // VT) * VT
    chunk = 2 * tok_dev
    n_vt = padded // VT
    half = tok_dev // 2
    f32, bf16 = jnp.float32, jnp.bfloat16
    hbm = pl.BlockSpec(memory_space=pltpu.MemorySpace.HBM)
    dma = pltpu.SemaphoreType.DMA
    return pl.pallas_call(
        head_kernel,
        out_shape=[
            jax.ShapeDtypeStruct((tokens, width), bf16),
            jax.ShapeDtypeStruct((padded, tokens), bf16),
            jax.ShapeDtypeStruct((half, 2 * width - EARLY), f32),
            jax.ShapeDtypeStruct((half, 2 * width - EARLY), f32),
            jax.ShapeDtypeStruct((tok_dev, width), f32),
            jax.ShapeDtypeStruct((3 * n_vt, VT, chunk), f32),
            jax.ShapeDtypeStruct((1, LANES), f32),
        ],
        in_specs=[hbm] * 5,
        out_specs=[hbm] * 7,
        scratch_shapes=[
            pltpu.VMEM((1, tok_dev), labels.dtype),
            *[pltpu.VMEM((1, count), f32) for count in (tok_dev, width, LANES)],
            pltpu.VMEM((padded, width), bf16),
            pltpu.VMEM((tokens, width), bf16),
            *[pltpu.VMEM((n_vt // 2, VT, chunk), f32) for _ in "eo"],
            *[pltpu.VMEM((chunk, padded), bf16) for _ in "eo"],
            pltpu.VMEM((8, 1, chunk), f32),
            pltpu.VMEM((8, tokens), f32),
            pltpu.VMEM((2, half, NT), f32),
            pltpu.VMEM((4, 2, 1, chunk), f32),
            pltpu.VMEM((8, 4, 1, 2 * chunk), f32),
            pltpu.VMEM((2, chunk, NT), f32),
            pltpu.VMEM((2, tok_dev, NT), f32),
            pltpu.VMEM((2, 2, half, NT), f32),
            pltpu.VMEM((2, tok_dev, NT), f32),
            *[pltpu.VMEM((2, 2, half, NT), f32) for _ in "hf"],
            *[dma((count,)) for count in (12, 7, 28, 2, 4, 2) for _ in "sr"],
            dma((5,)), dma((n_vt,)), dma((n_vt,)), dma((4,)), dma((4,)), dma((10,)),
            pltpu.SemaphoreType.REGULAR,
        ],
        compiler_params=pltpu.CompilerParams(
            collective_id=0, has_side_effects=True, vmem_limit_bytes=VMEM_BYTES,
        ),
        cost_estimate=pl.CostEstimate(
            flops=4 * tokens * width * padded, bytes_accessed=120_000_000, transcendentals=2 * tokens * padded
        ),
        name="head",
    )(hidden, labels[None], loss_weight[None], norm_gain[None], w_t)


def tail_kernel(
    h_v, gain_ref, own_v, x_v, y_v, loss_ref, dh_v, dgain_ref, total_ref, g_v, buf, send, recv
):
    me = lax.axis_index("vp")
    peers = xor_peers(me)
    barrier = pltpu.get_barrier_semaphore()
    for r in OTHERS:
        pl.semaphore_signal(barrier, inc=1, device_id={"vp": peers[r]}, device_id_type=MESH)
    rows, width = h_v.shape
    half = rows // 2
    rest_at = x_v.shape[1] - width
    early = width - rest_at
    acc = jnp.zeros((SUBLANES, width), jnp.float32)
    for b in range(0, rows, 32):
        at = slice(b, b + 32)
        here = slice(b % half, b % half + 32)
        part, rest = (x_v, y_v) if b < half else (y_v, x_v)
        x = h_v[at, :].astype(jnp.float32)
        inv_rms = lax.rsqrt(jnp.mean(x * x, axis=-1, keepdims=True) + NORM_EPS)
        own = own_v[at, :] + rest[here, rest_at:rest_at + width]
        g = jnp.concatenate([own[:, :early], own[:, early:] + part[here, :rest_at]], axis=1)
        g_v[at, :] = g
        gn = g * (x * inv_rms)
        for i in range(0, 32, 8):
            acc += gn[i:i + 8, :]
    buf[0, :, :width] = jnp.sum(acc, axis=0, keepdims=True)
    buf[0, :, width:width + LANES] = loss_ref[...]
    pl.semaphore_wait(barrier, 7)
    copies = [
        pltpu.make_async_remote_copy(
            src_ref=buf.at[0], dst_ref=buf.at[r], send_sem=send.at[r - 1], recv_sem=recv.at[r - 1],
            device_id={"vp": peers[r]}, device_id_type=MESH,
        )
        for r in OTHERS
    ]
    for copy in copies:
        copy.start()
    for b in range(0, rows, 32):
        at = slice(b, b + 32)
        x = h_v[at, :].astype(jnp.float32)
        inv_rms = lax.rsqrt(jnp.mean(x * x, axis=-1, keepdims=True) + NORM_EPS)
        n = x * inv_rms
        u = g_v[at, :] * gain_ref[...]
        dh_v[at, :] = (inv_rms * (u - n * jnp.mean(u * n, axis=-1, keepdims=True))).astype(jnp.bfloat16)
    for copy in copies:
        copy.wait()
    pairs = [buf[2 * r] + buf[2 * r + 1] for r in range(4)]
    total = (pairs[0] + pairs[1]) + (pairs[2] + pairs[3])
    dgain_ref[...] = total[:, :width]
    total_ref[...] = jnp.broadcast_to(jnp.sum(total[:, width:], axis=1, keepdims=True), total_ref.shape)


def tail(hidden, norm_gain, own, from_x, from_y, loss):
    tok_dev, width = hidden.shape
    whole = pl.BlockSpec(memory_space=pltpu.VMEM)
    return pl.pallas_call(
        tail_kernel,
        out_shape=[
            jax.ShapeDtypeStruct((tok_dev, width), jnp.bfloat16),
            jax.ShapeDtypeStruct((1, width), jnp.float32),
            jax.ShapeDtypeStruct((1, LANES), jnp.float32),
        ],
        in_specs=[whole] * 6,
        out_specs=[whole] * 3,
        scratch_shapes=[
            pltpu.VMEM((tok_dev, width), jnp.float32),
            pltpu.VMEM((8, 1, width + LANES), jnp.float32),
            *[pltpu.SemaphoreType.DMA((7,)) for _ in "sr"],
        ],
        compiler_params=pltpu.CompilerParams(collective_id=1, has_side_effects=True, vmem_limit_bytes=SMALL_BYTES),
        cost_estimate=pl.CostEstimate(flops=10 * tok_dev * width, bytes_accessed=8_000_000, transcendentals=0),
        name="tail",
    )(hidden, norm_gain[None], own, from_x, from_y, loss)


def finish_kernel(dh_ref, dgain_ref, loss_ref, dh_out, dgain_out, loss_out):
    dh_out[...] = dh_ref[...]
    dgain_out[...] = dgain_ref[...]
    loss_out[...] = loss_ref[:, :1]


def finish(dh, dgain, loss):
    whole = pl.BlockSpec(memory_space=pltpu.VMEM)
    return pl.pallas_call(
        finish_kernel,
        out_shape=[
            jax.ShapeDtypeStruct(dh.shape, dh.dtype),
            jax.ShapeDtypeStruct(dgain.shape, dgain.dtype),
            jax.ShapeDtypeStruct((1, 1), loss.dtype),
        ],
        in_specs=[whole] * 3,
        out_specs=[whole] * 3,
        compiler_params=pltpu.CompilerParams(vmem_limit_bytes=SMALL_BYTES),
        name="finish",
    )(dh, dgain, loss)


def weight_grad_kernel(dz_hbm, a_hbm, out_hbm, dz_v, a_v, out_v, dz_sem, a_sem, out_sem):
    vocab_local = out_hbm.shape[0]
    n_vt = dz_hbm.shape[0] // VT

    def dz_copy(v):
        return pltpu.make_async_copy(
            dz_hbm.at[pl.ds(pl.multiple_of(v * VT, VT), VT)], dz_v.at[v % 2], dz_sem.at[v % 2]
        )

    def a_copy(d):
        return pltpu.make_async_copy(a_hbm.at[:, d * NT:(d + 1) * NT], a_v.at[:, d * NT:(d + 1) * NT], a_sem.at[d])

    def out_copy(v, d, count):
        return pltpu.make_async_copy(
            out_v.at[d, :count],
            out_hbm.at[pl.ds(pl.multiple_of(v * VT, VT), count), pl.ds(pl.multiple_of(d * NT, NT), NT)],
            out_sem.at[d],
        )

    last_count = vocab_local - (n_vt - 1) * VT
    dz_copy(0).start()
    a_copy(0).start()

    def step(i, carry):
        v, d = i // 2, i % 2

        @pl.when(d == 0)
        def _():
            dz_copy(v).wait()

        for dd in range(2):
            @pl.when(i == dd)
            def _():
                a_copy(dd).wait()
                if dd == 0:
                    a_copy(1).start()
                    dz_copy(1).start()

        @pl.when(i >= 2)
        def _():
            out_copy(v - 1, d, VT).wait()

        cols = pl.ds(pl.multiple_of(d * NT, NT), NT)
        out_v[d] = jnp.dot(dz_v[v % 2], a_v[:, cols], preferred_element_type=jnp.float32)

        @pl.when(v < n_vt - 1)
        def _():
            out_copy(v, d, VT).start()

        @pl.when(v == n_vt - 1)
        def _():
            out_copy(v, d, last_count).start()

        @pl.when((d == 1) & (v < n_vt - 2))
        def _():
            dz_copy(v + 2).start()

        return carry

    lax.fori_loop(0, 2 * n_vt, step, 0)
    for d in range(2):
        out_copy(n_vt - 1, d, last_count).wait()


def weight_grad(dz_t, a_all, vocab_local):
    tokens, width = a_all.shape
    padded = dz_t.shape[0]
    hbm = pl.BlockSpec(memory_space=pltpu.MemorySpace.HBM)
    return pl.pallas_call(
        weight_grad_kernel,
        out_shape=jax.ShapeDtypeStruct((vocab_local, width), jnp.float32),
        in_specs=[hbm, hbm],
        out_specs=hbm,
        scratch_shapes=[
            pltpu.VMEM((2, VT, tokens), jnp.bfloat16),
            pltpu.VMEM((tokens, width), jnp.bfloat16),
            pltpu.VMEM((2, VT, NT), jnp.float32),
            *[pltpu.SemaphoreType.DMA((2,)) for _ in "dao"],
        ],
        compiler_params=pltpu.CompilerParams(vmem_limit_bytes=59_000_000),
        cost_estimate=pl.CostEstimate(
            flops=2 * tokens * width * padded, bytes_accessed=60_000_000, transcendentals=0
        ),
        name="weight_grad",
    )(dz_t, a_all)


def solution(mesh):
    group_size = mesh.shape["vp"]

    def local_step(hidden, labels, loss_weight, norm_gain, w_local):
        vocab_local = w_local.shape[1]
        a_all, dz_t, px, py, pown, _, loss = head(hidden, labels, loss_weight, norm_gain, w_local.T)
        from_x = lax.ppermute(px, "vp", [(i, i ^ 2) for i in range(group_size)])
        from_y = lax.ppermute(py, "vp", [(i, i ^ 4) for i in range(group_size)])
        d_unembed = weight_grad(dz_t, a_all, vocab_local).T
        small = tail(hidden, norm_gain, pown, from_x, from_y, loss)
        d_input, d_gain, mean_loss = finish(*small)
        return mean_loss[0], d_input, d_unembed, d_gain[0]

    return jax.shard_map(
        local_step,
        mesh=mesh,
        in_specs=(P(("dp", "vp"), None), P(("dp", "vp")), P(("dp", "vp")), P(None), P(None, "vp")),
        out_specs=(P("dp"), P(("dp", "vp"), None), P("dp", "vp"), P("dp")),
        check_vma=False,
    )
```
